768 devices in a mesh: aa: 12 (over z), ba: 64 (over y, x, core).
Axes of the slice: x: 4, y: 8, z: 12, core: 2. Of those that a mesh axis runs over, the one named last changes fastest.
Arguments:
- grad_out: bfloat16 [98304, 4096], P('aa', 'ba')
- saved_input: bfloat16 [98304, 4096], P(('aa', 'ba'))
- keep_bits: int32 [98304, 128], P(('aa', 'ba')), may hold values from -2147483648 to 2147483647, as said below
- gain: float32 [4096], replicated, may hold values from 0.5 to 1.5
Outputs:
- grad_in: bfloat16 [98304, 4096], P(('aa', 'ba'))
- gain_grad: float32 [4096], P('ba')
The draws below stay inside these ranges and needn't reach their ends.
Inputs may be any that keep to these rules, and one draw needn't show every extreme that they name: `keep_bits`: bit k of word w in row t (bit 31 being the sign bit) is the keep flag of feature 32 * w + k of token t; about nine in ten flags are 1.
All inputs are finite; a program needn't handle non-finite values.
Results may differ from the reference program's by a relative error of at most 0.001.
Values may be sent and summed in bfloat16 or wider, within the bound.
A program may use at most 32 MiB of HBM per device.

```python
import math
import jax
import jax.numpy as jnp
from jax import lax

D = 4096
TOKENS = 98304
WORDS = 128


def draw_grad_out(key, part):
    first = jax.random.fold_in(key, 11)
    second = jax.random.fold_in(key, 12)
    rise = 1.0 + 2.0 * jnp.arange(TOKENS, dtype=jnp.float32) / TOKENS
    rough = jnp.exp(jax.random.uniform(second, (TOKENS,), jnp.float32, jnp.log(0.5), jnp.log(2.0)))
    base = jax.random.normal(first, (TOKENS, D), jnp.float32)
    values = base * (rise * rough)[:, None]
    return values.astype(jnp.bfloat16)


def draw_saved_input(key, part):
    first = jax.random.fold_in(key, 21)
    second = jax.random.fold_in(key, 22)
    third = jax.random.fold_in(key, 23)
    base = jax.random.normal(first, (TOKENS, D), jnp.float32)
    row_scale = jnp.exp(jax.random.uniform(second, (TOKENS,), jnp.float32, jnp.log(0.3), jnp.log(3.0)))
    column_scale = jnp.exp(jax.random.uniform(third, (D,), jnp.float32, jnp.log(0.5), jnp.log(5.0)))
    values = base * row_scale[:, None] * column_scale[None, :]
    return values.astype(jnp.bfloat16)


def draw_keep_bits(key, part):
    picks = jax.random.randint(jax.random.fold_in(key, 31), (TOKENS, WORDS, 32), 0, 10)
    flags = (picks < 9).astype(jnp.int32)
    shifts = jnp.arange(32, dtype=jnp.int32)
    return jnp.sum(jnp.left_shift(flags, shifts[None, None, :]), axis=-1).astype(jnp.int32)


def setup_inputs(seed: int = 0) -> dict:
    seeds = jax.random.split(jax.random.key(seed), 5)
    grad_out = draw_grad_out(jax.random.fold_in(seeds[4], 71), 0)
    saved_input = draw_saved_input(jax.random.fold_in(seeds[4], 71), 0)
    keep_bits = draw_keep_bits(jax.random.fold_in(seeds[4], 71), 0)
    gain = jnp.clip(1.0 + 0.1 * jax.random.normal(seeds[3], (D,), jnp.float32), 0.5, 1.5)
    return {"grad_out": grad_out, "saved_input": saved_input, "keep_bits": keep_bits, "gain": gain}


KEEP_RATE = 0.9
EPSILON = 1e-06

def unpack_bits(words):
    shifts = jnp.arange(32, dtype=jnp.int32)
    bits = jnp.right_shift(words[:, :, None], shifts[None, None, :]) & 1
    return bits.reshape(words.shape[0], words.shape[1] * 32).astype(jnp.float32)

def rows_backward(grad_rows, input_rows, word_rows, gain):
    keep = unpack_bits(word_rows)
    dropped = input_rows.astype(jnp.float32) * keep * (1.0 / KEEP_RATE)
    inverse = lax.rsqrt(lax.optimization_barrier(jnp.mean(dropped * dropped, axis=-1, keepdims=True)) + EPSILON)
    normed = dropped * inverse
    grads = grad_rows.astype(jnp.float32)
    scaled = gain[None, :] * grads
    centre = lax.optimization_barrier(jnp.mean(scaled * normed, axis=-1, keepdims=True))
    grad_in = (inverse * (scaled - normed * centre) * keep * (1.0 / KEEP_RATE)).astype(jnp.bfloat16)
    partial_sum = lax.optimization_barrier(jnp.sum(grads * normed, axis=0))
    return (grad_in, partial_sum)

def reference(grad_out, saved_input, keep_bits, gain):
    block = math.gcd(TOKENS, 512)
    count = TOKENS // block

    def one_block(items):
        return rows_backward(items[0], items[1], items[2], gain)
    grad_in, partial_sums = lax.map(one_block, (grad_out.reshape(count, block, D), saved_input.reshape(count, block, D), keep_bits.reshape(count, block, WORDS)))
    gain_grad = lax.optimization_barrier(jnp.sum(partial_sums, axis=0)) * (1.0 / math.sqrt(TOKENS))
    return (grad_in.reshape(TOKENS, D), gain_grad)
```

```python
import functools
import math

import jax
import jax.numpy as jnp
from jax import lax
from jax.experimental import pallas as pl
from jax.experimental.pallas import tpu as pltpu
from jax.sharding import PartitionSpec as P

KEEP_RATE = 0.9
EPSILON = 1e-06
MESH = pl.DeviceIdType.MESH
LANES = 128
NY, NX, NC = 8, 4, 2
CHIPS = NY * NX
PEERS = CHIPS * NC


def offset(r):
    def far_first(i, n):
        return n // 2 + (1 - 2 * lax.rem(i, 2)) * lax.div(i + 1, 2)

    return far_first(lax.rem(r, NY), NY), far_first(lax.div(r, NY), NX)


def exchange_kernel(
    gt_hbm, x_hbm, kb_hbm, gain_ref, gin_ref, own_ref,
    x_ref, kb_ref, recv, keep_ref, n_ref, gs_ref, part, ret, acc,
    in_sem, send_sem, recv_sem, psend_sem, pret_sem,
):
    me = lax.axis_index("ba")
    core = lax.rem(me, NC)
    chip = lax.div(me, NC)
    my_y, my_x = lax.div(chip, NX), lax.rem(chip, NX)

    barrier = pltpu.get_barrier_semaphore()

    def greet(o, _):
        pl.semaphore_signal(barrier, inc=1, device_id={"ba": lax.rem(me + o, PEERS)}, device_id_type=MESH)
        return 0

    lax.fori_loop(1, PEERS, greet, 0)
    load_x = pltpu.make_async_copy(x_hbm, x_ref, in_sem.at[0])
    load_kb = pltpu.make_async_copy(kb_hbm, kb_ref, in_sem.at[1])
    load_x.start()
    load_kb.start()
    load_own = pltpu.make_async_copy(
        gt_hbm.at[:, pl.ds(pl.multiple_of(me * LANES, LANES), LANES)], recv.at[me], in_sem.at[2])
    load_own.start()
    pl.semaphore_wait(barrier, PEERS - 1)

    def target(r):
        dy, dx = offset(r)
        return lax.rem(my_y + dy, NY) * NX + lax.rem(my_x + dx, NX)

    def source(r):
        dy, dx = offset(r)
        return lax.rem(my_y - dy + NY, NY) * NX + lax.rem(my_x - dx + NX, NX)

    def bulk(r, dst):
        return pltpu.make_async_remote_copy(
            gt_hbm.at[:, pl.ds(pl.multiple_of(dst * LANES, LANES), LANES)],
            recv.at[me], send_sem, recv_sem.at[r],
            device_id={"ba": dst}, device_id_type=MESH)

    def send(r, _):
        to = target(r) * NC
        bulk(r, to).start()
        bulk(r, to + 1).start()
        return 0

    lax.fori_loop(0, CHIPS - 1, send, 0)
    bulk(CHIPS - 1, chip * NC + (1 - core)).start()

    lane = lax.broadcasted_iota(jnp.int32, (LANES, LANES), 1)
    word = lax.div(lane, 32)
    shift = 31 - lax.rem(lane, 32)
    load_x.wait()
    load_kb.wait()
    acc[...] = jnp.zeros_like(acc)

    def forward(k, _):
        x = x_ref[:, pl.ds(pl.multiple_of(k * LANES, LANES), LANES)].astype(jnp.float32)
        words = jnp.take_along_axis(kb_ref[...], word + 4 * k, axis=1)
        keep = jnp.where(jnp.left_shift(words, shift) < 0, 1.0, 0.0)
        dropped = x * keep * (1.0 / KEEP_RATE)
        keep_ref[k] = keep
        n_ref[k] = dropped
        acc[...] += dropped * dropped
        return 0

    lax.fori_loop(0, CHIPS, forward, 0)
    mean = jnp.sum(acc[...], axis=1, keepdims=True) * (1.0 / (CHIPS * LANES))
    inverse = lax.rsqrt(mean + EPSILON)

    def normalise(k, _):
        n_ref[k] = n_ref[k] * inverse
        return 0

    lax.fori_loop(0, CHIPS, normalise, 0)
    acc[...] = jnp.zeros_like(acc)

    def give_back(r):
        k = source(r)
        return pltpu.make_async_remote_copy(
            part.at[pl.ds(r, 1)], ret.at[pl.ds(chip, 1)], psend_sem, pret_sem,
            device_id={"ba": k * NC + core}, device_id_type=MESH)

    def block(r):
        k = source(r)
        grads = recv[pl.ds(k * NC, NC)].reshape(LANES, LANES).astype(jnp.float32).T
        grads = grads * keep_ref[k]
        normed = n_ref[k]
        part[pl.ds(r, 1), :] = jnp.sum(grads * normed, axis=0, keepdims=True)
        scaled = grads * gain_ref[pl.ds(k, 1), :]
        gs_ref[k] = scaled
        acc[...] += scaled * normed

    def arrive(r, _):
        both = recv.at[pl.ds(0, NC)]
        pltpu.make_async_copy(both, both, recv_sem.at[r]).wait()
        block(r)
        give_back(r).start()
        return 0

    lax.fori_loop(0, CHIPS - 1, arrive, 0)
    last = CHIPS - 1
    one = recv.at[0]
    pltpu.make_async_copy(one, one, recv_sem.at[last]).wait()
    load_own.wait()
    block(last)
    ret[pl.ds(chip, 1), :] = part[pl.ds(last, 1), :]

    centre = jnp.sum(acc[...], axis=1, keepdims=True) * (1.0 / (CHIPS * LANES))
    a = inverse * (1.0 / KEEP_RATE)
    b = a * centre
    for k in range(CHIPS):
        gin_ref[:, k * LANES:(k + 1) * LANES] = (a * gs_ref[k] - b * n_ref[k]).astype(jnp.bfloat16)

    rest = ret.at[pl.ds(0, CHIPS - 1)]
    pltpu.make_async_copy(rest, rest, pret_sem).wait()
    own_ref[...] = jnp.broadcast_to(jnp.sum(ret[...], axis=0, keepdims=True), own_ref.shape)
    pltpu.make_async_copy(rest, rest, psend_sem).wait()
    sent = recv.at[pl.ds(0, PEERS - 1)]
    pltpu.make_async_copy(sent, sent, send_sem).wait()


def total_kernel(planes, scale, own_ref, out_ref, buf, send_sem, recv_sem):
    me = lax.axis_index("ba")
    plane = lax.axis_index("aa")
    core = lax.rem(me, NC)
    mine = plane * NC + core
    everyone = planes * NC

    def peer(o):
        p = lax.rem(mine + o, everyone)
        return {"aa": lax.div(p, NC), "ba": me - core + lax.rem(p, NC)}

    barrier = pltpu.get_barrier_semaphore()

    def greet(o, _):
        pl.semaphore_signal(barrier, inc=1, device_id=peer(o), device_id_type=MESH)
        return 0

    lax.fori_loop(1, everyone, greet, 0)
    pl.semaphore_wait(barrier, everyone - 1)

    def send(o, _):
        pltpu.make_async_remote_copy(
            own_ref.at[pl.ds(0, 1)], buf.at[pl.ds(mine, 1)], send_sem, recv_sem,
            device_id=peer(o), device_id_type=MESH).start()
        return 0

    lax.fori_loop(1, everyone, send, 0)
    buf[pl.ds(mine, 1), :] = own_ref[pl.ds(0, 1), :]
    rest = buf.at[pl.ds(0, everyone - 1)]
    pltpu.make_async_copy(rest, rest, recv_sem).wait()
    total = jnp.sum(buf[...], axis=0, keepdims=True) * scale
    half = LANES // NC
    out_ref[...] = jnp.where(core == 0, total[:, :half], total[:, half:])
    pltpu.make_async_copy(rest, rest, send_sem).wait()


def per_device(planes, grad_out, saved_input, keep_bits, gain):
    rows, width = saved_input.shape
    tokens = grad_out.shape[0] * planes
    vmem = functools.partial(pl.BlockSpec, memory_space=pltpu.VMEM)
    hbm = functools.partial(pl.BlockSpec, memory_space=pl.ANY)
    f32 = jnp.float32
    grad_in, own = pl.pallas_call(
        exchange_kernel,
        name="exchange",
        out_shape=(jax.ShapeDtypeStruct((rows, width), jnp.bfloat16), jax.ShapeDtypeStruct((8, LANES), f32)),
        in_specs=[hbm(), hbm(), hbm(), vmem()],
        out_specs=(vmem(), vmem()),
        scratch_shapes=[
            pltpu.VMEM((rows, width), jnp.bfloat16),
            pltpu.VMEM(keep_bits.shape, jnp.int32),
            pltpu.VMEM((PEERS, LANES // NC, LANES), jnp.bfloat16),
            pltpu.VMEM((CHIPS, LANES, LANES), f32),
            pltpu.VMEM((CHIPS, LANES, LANES), f32),
            pltpu.VMEM((CHIPS, LANES, LANES), f32),
            pltpu.VMEM((CHIPS, LANES), f32),
            pltpu.VMEM((CHIPS, LANES), f32),
            pltpu.VMEM((LANES, LANES), f32),
            pltpu.SemaphoreType.DMA((3,)),
            pltpu.SemaphoreType.DMA,
            pltpu.SemaphoreType.DMA((CHIPS,)),
            pltpu.SemaphoreType.DMA,
            pltpu.SemaphoreType.DMA,
        ],
        compiler_params=pltpu.CompilerParams(collective_id=0, has_side_effects=True, vmem_limit_bytes=24 << 20),
    )(grad_out.T, saved_input, keep_bits, gain.reshape(CHIPS, LANES))
    share = pl.pallas_call(
        functools.partial(total_kernel, planes, 1.0 / math.sqrt(tokens)),
        name="total",
        out_shape=jax.ShapeDtypeStruct((1, LANES // NC), f32),
        in_specs=[vmem()],
        out_specs=vmem(),
        scratch_shapes=[pltpu.VMEM((planes * NC, LANES), f32), pltpu.SemaphoreType.DMA, pltpu.SemaphoreType.DMA],
        compiler_params=pltpu.CompilerParams(collective_id=1, has_side_effects=True, vmem_limit_bytes=1 << 20),
    )(own)
    return grad_in, share.reshape(LANES // NC)


def solution(mesh):
    placed = (P("aa", "ba"), P(("aa", "ba"), None), P(("aa", "ba"), None), P())
    return jax.shard_map(
        functools.partial(per_device, mesh.shape["aa"]),
        mesh=mesh,
        in_specs=placed,
        out_specs=(P(("aa", "ba"), None), P("ba")),
        check_vma=False,
    )
```

```python
import functools
import math

import jax
import jax.numpy as jnp
from jax import lax
from jax.experimental import pallas as pl
from jax.experimental.pallas import tpu as pltpu
from jax.sharding import PartitionSpec as P

KEEP_RATE = 0.9
EPSILON = 1e-06
MESH = pl.DeviceIdType.MESH
LANES = 128
NY, NX, NC = 8, 4, 2
CHIPS = NY * NX
PEERS = CHIPS * NC


def far_first(i, n):
    return n // 2 + (1 - 2 * (i & 1)) * ((i + 1) >> 1)


def offset(r):
    return far_first(r & (NY - 1), NY), far_first(r >> 3, NX)


def exchange_kernel(
    planes, scale,
    gt_hbm, x_hbm, kb_hbm, gain_hbm, gin_ref, total_ref,
    x_ref, kb_ref, gain_ref, recv, keep_ref, n_ref, gs_ref, part, ret, column, acc,
    in_sem, send_sem, recv_sem, psend_sem, pret_sem, csend_sem, crecv_sem,
):
    me = lax.axis_index("ba")
    plane = lax.axis_index("aa")
    core = me & 1
    chip = me >> 1
    my_y, my_x = chip >> 2, chip & (NX - 1)
    everyone = planes * NC
    mine = plane * NC + core

    def in_column(o):
        p = lax.rem(mine + o, everyone)
        return {"aa": p >> 1, "ba": me - core + (p & 1)}

    barrier = pltpu.get_barrier_semaphore()

    def greet_plane(o, _):
        pl.semaphore_signal(barrier, inc=1, device_id={"ba": (me + o) & (PEERS - 1)}, device_id_type=MESH)
        return 0

    def greet_column(o, _):
        p = lax.rem(plane + (o >> 1), planes)
        pl.semaphore_signal(barrier, inc=1, device_id={"aa": p, "ba": me - core + (o & 1)}, device_id_type=MESH)
        return 0

    lax.fori_loop(NC, everyone, greet_column, 0)
    lax.fori_loop(1, PEERS, greet_plane, 0)
    loads = [
        pltpu.make_async_copy(x_hbm, x_ref, in_sem.at[0]),
        pltpu.make_async_copy(kb_hbm, kb_ref, in_sem.at[1]),
        pltpu.make_async_copy(gain_hbm, gain_ref, in_sem.at[2]),
        pltpu.make_async_copy(
            gt_hbm.at[:, pl.ds(pl.multiple_of(me * LANES, LANES), LANES)], recv.at[me], in_sem.at[3]),
    ]
    for load in loads:
        load.start()
    pl.semaphore_wait(barrier, PEERS - 1 + everyone - NC)

    def target(r):
        dy, dx = offset(r)
        return ((my_y + dy) & (NY - 1)) * NX + ((my_x + dx) & (NX - 1))

    def source(r):
        dy, dx = offset(r)
        return ((my_y - dy) & (NY - 1)) * NX + ((my_x - dx) & (NX - 1))

    def bulk(r, dst):
        return pltpu.make_async_remote_copy(
            gt_hbm.at[:, pl.ds(pl.multiple_of(dst * LANES, LANES), LANES)],
            recv.at[me], send_sem, recv_sem.at[r],
            device_id={"ba": dst}, device_id_type=MESH)

    def send(r, _):
        to = target(r) * NC
        bulk(r, to).start()
        bulk(r, to + 1).start()
        return 0

    lax.fori_loop(0, CHIPS - 1, send, 0)
    bulk(CHIPS - 1, chip * NC + (1 - core)).start()

    lane = lax.broadcasted_iota(jnp.int32, (LANES, LANES), 1)
    word = lane >> 5
    shift = 31 - (lane & 31)
    for load in loads[:3]:
        load.wait()
    acc[...] = jnp.zeros_like(acc)

    def forward(k, _):
        x = x_ref[:, pl.ds(pl.multiple_of(k * LANES, LANES), LANES)].astype(jnp.float32)
        words = jnp.take_along_axis(kb_ref[...], word + 4 * k, axis=1)
        keep = jnp.where(jnp.left_shift(words, shift) < 0, 1.0, 0.0)
        dropped = x * keep * (1.0 / KEEP_RATE)
        keep_ref[k] = keep
        n_ref[k] = dropped
        acc[...] += dropped * dropped
        return 0

    lax.fori_loop(0, CHIPS, forward, 0)
    mean = jnp.sum(acc[...], axis=1, keepdims=True) * (1.0 / (CHIPS * LANES))
    inverse = lax.rsqrt(mean + EPSILON)

    def normalise(k, _):
        n_ref[k] = n_ref[k] * inverse
        return 0

    lax.fori_loop(0, CHIPS, normalise, 0)
    acc[...] = jnp.zeros_like(acc)

    def give_back(r):
        return pltpu.make_async_remote_copy(
            part.at[pl.ds(r, 1)], ret.at[pl.ds(chip, 1)], psend_sem, pret_sem,
            device_id={"ba": source(r) * NC + core}, device_id_type=MESH)

    def block(r):
        k = source(r)
        grads = recv[pl.ds(k * NC, NC)].reshape(LANES, LANES).astype(jnp.float32).T
        grads = grads * keep_ref[k]
        normed = n_ref[k]
        part[pl.ds(r, 1), :] = jnp.sum(grads * normed, axis=0, keepdims=True)
        scaled = grads * gain_ref[pl.ds(k, 1), :]
        gs_ref[k] = scaled
        acc[...] += scaled * normed

    def arrive(r, _):
        both = recv.at[pl.ds(0, NC)]
        pltpu.make_async_copy(both, both, recv_sem.at[r]).wait()
        block(r)
        give_back(r).start()
        return 0

    lax.fori_loop(0, CHIPS - 1, arrive, 0)
    last = CHIPS - 1
    one = recv.at[0]
    pltpu.make_async_copy(one, one, recv_sem.at[last]).wait()
    loads[3].wait()
    block(last)
    ret[pl.ds(chip, 1), :] = part[pl.ds(last, 1), :]

    centre = jnp.sum(acc[...], axis=1, keepdims=True) * (1.0 / (CHIPS * LANES))
    a = inverse * (1.0 / KEEP_RATE)
    b = a * centre

    def finish(k, _):
        gin_ref[:, pl.ds(pl.multiple_of(k * LANES, LANES), LANES)] = (a * gs_ref[k] - b * n_ref[k]).astype(jnp.bfloat16)
        return 0

    lax.fori_loop(0, CHIPS, finish, 0)

    rest = ret.at[pl.ds(0, CHIPS - 1)]
    pltpu.make_async_copy(rest, rest, pret_sem).wait()
    column[pl.ds(mine, 1), :] = jnp.sum(ret[...], axis=0, keepdims=True)

    def tell(o, _):
        pltpu.make_async_remote_copy(
            column.at[pl.ds(mine, 1)], column.at[pl.ds(mine, 1)], csend_sem, crecv_sem,
            device_id=in_column(o), device_id_type=MESH).start()
        return 0

    lax.fori_loop(1, everyone, tell, 0)
    pltpu.make_async_copy(rest, rest, psend_sem).wait()
    sent = recv.at[pl.ds(0, PEERS - 1)]
    pltpu.make_async_copy(sent, sent, send_sem).wait()
    others = column.at[pl.ds(0, everyone - 1)]
    pltpu.make_async_copy(others, others, csend_sem).wait()
    pltpu.make_async_copy(others, others, crecv_sem).wait()
    total = jnp.sum(column[...], axis=0, keepdims=True) * scale
    half = LANES // NC
    total_ref[...] = jnp.where(core == 0, total[:, :half], total[:, half:])


def write_kernel(gin_ref, total_ref, gin_hbm, gain_hbm, sems):
    copies = [pltpu.make_async_copy(gin_ref, gin_hbm, sems.at[0]), pltpu.make_async_copy(total_ref, gain_hbm, sems.at[1])]
    for copy in copies:
        copy.start()
    for copy in copies:
        copy.wait()


def per_device(planes, grad_out, saved_input, keep_bits, gain):
    rows, width = saved_input.shape
    tokens = grad_out.shape[0] * planes
    vmem = functools.partial(pl.BlockSpec, memory_space=pltpu.VMEM)
    hbm = functools.partial(pl.BlockSpec, memory_space=pltpu.HBM)
    f32 = jnp.float32
    grad_in = jax.ShapeDtypeStruct((rows, width), jnp.bfloat16)
    share = jax.ShapeDtypeStruct((1, LANES // NC), f32)
    blocks = pltpu.VMEM((CHIPS, LANES, LANES), f32)
    results = pl.pallas_call(
        functools.partial(exchange_kernel, planes, 1.0 / math.sqrt(tokens)),
        name="exchange",
        out_shape=(pltpu.VMEM(grad_in.shape, grad_in.dtype), pltpu.VMEM(share.shape, f32)),
        in_specs=[hbm(), hbm(), hbm(), hbm()],
        out_specs=(vmem(), vmem()),
        scratch_shapes=[
            pltpu.VMEM((rows, width), jnp.bfloat16),
            pltpu.VMEM(keep_bits.shape, jnp.int32),
            pltpu.VMEM((CHIPS, LANES), f32),
            pltpu.VMEM((PEERS, LANES // NC, LANES), jnp.bfloat16),
            blocks, blocks, blocks,
            pltpu.VMEM((CHIPS, LANES), f32),
            pltpu.VMEM((CHIPS, LANES), f32),
            pltpu.VMEM((planes * NC, LANES), f32),
            pltpu.VMEM((LANES, LANES), f32),
            pltpu.SemaphoreType.DMA((4,)),
            pltpu.SemaphoreType.DMA,
            pltpu.SemaphoreType.DMA((CHIPS,)),
            pltpu.SemaphoreType.DMA,
            pltpu.SemaphoreType.DMA,
            pltpu.SemaphoreType.DMA,
            pltpu.SemaphoreType.DMA,
        ],
        compiler_params=pltpu.CompilerParams(collective_id=0, has_side_effects=True, vmem_limit_bytes=24 << 20),
    )(*(pltpu.with_memory_space_constraint(a, pltpu.HBM) for a in (grad_out.T, saved_input, keep_bits, gain.reshape(CHIPS, LANES))))
    grad_in, share = pl.pallas_call(
        write_kernel,
        name="write",
        out_shape=(grad_in, share),
        in_specs=[vmem(), vmem()],
        out_specs=(hbm(), hbm()),
        scratch_shapes=[pltpu.SemaphoreType.DMA((2,))],
        compiler_params=pltpu.CompilerParams(vmem_limit_bytes=4 << 20),
    )(*results)
    return grad_in, share.reshape(LANES // NC)


def solution(mesh):
    placed = (P("aa", "ba"), P(("aa", "ba"), None), P(("aa", "ba"), None), P())
    return jax.shard_map(
        functools.partial(per_device, mesh.shape["aa"]),
        mesh=mesh,
        in_specs=placed,
        out_specs=(P(("aa", "ba"), None), P("ba")),
        check_vma=False,
    )
```

```python
import functools
import math

import jax
import jax.numpy as jnp
from jax import lax
from jax.experimental import pallas as pl
from jax.experimental.pallas import tpu as pltpu
from jax.sharding import PartitionSpec as P

KEEP_RATE = 0.9
EPSILON = 1e-06
MESH = pl.DeviceIdType.MESH
LANES = 128
NY, NX, NC = 8, 4, 2
CHIPS = NY * NX
PEERS = CHIPS * NC


STAGES = (
    (0, 0, ((0, 2), (0, 1), (0, 3))),
    (1, 1, ((1, 2), (7, 2))),
    (2, 2, ((2, 2), (6, 2))),
    (3, 3, ((3, 2), (5, 2))),
    (4, 3, ((4, 2), (4, 1), (3, 1), (5, 1), (2, 1), (6, 1), (1, 1), (7, 1), (4, 3), (3, 3), (5, 3), (2, 3), (6, 3), (1, 3), (7, 3),
            (4, 0), (3, 0), (5, 0), (2, 0), (6, 0), (1, 0), (7, 0))),
)
ORDER = tuple(o for _, _, offsets in STAGES for o in offsets)
PER_WORD = 6


def offset(r):
    codes = [dy * NX + dx for dy, dx in ORDER]
    words = [sum(c << (5 * i) for i, c in enumerate(codes[w:w + PER_WORD])) for w in range(0, len(codes), PER_WORD)]
    group = r // PER_WORD
    word = jnp.int32(words[0])
    for g, w in enumerate(words[1:], 1):
        word = jnp.where(group >= g, jnp.int32(w), word)
    code = (word >> (5 * (r - group * PER_WORD))) & (CHIPS - 1)
    return code >> 2, code & (NX - 1)


def exchange_kernel(
    planes, scale,
    gt_hbm, x_hbm, kb_hbm, gain_hbm, gin_ref, total_ref,
    x_ref, kb_ref, gain_ref, recv, keep_ref, n_ref, gs_ref, part, ret, column, acc,
    in_sem, send_sem, recv_sem, psend_sem, pret_sem, csend_sem, crecv_sem, ahead_sem, behind_sem, above_sem, below_sem,
):
    me = lax.axis_index("ba")
    plane = lax.axis_index("aa")
    core = me & 1
    chip = me >> 1
    my_y, my_x = chip >> 2, chip & (NX - 1)
    everyone = planes * NC
    mine = plane * NC + core

    def at(dy, dx=0):
        return ((my_y + dy) & (NY - 1)) * NX + ((my_x + dx) & (NX - 1))

    def ahead(dy):
        return {"ba": at(dy) * NC + core}

    def above(dz):
        return {"aa": lax.rem(plane + dz + planes, planes)}

    def signal(sem, device):
        pl.semaphore_signal(sem, inc=1, device_id=device, device_id_type=MESH)

    barrier = pltpu.get_barrier_semaphore()
    row = NX * NC
    for device in (ahead(1), ahead(-1), above(1), above(-1)):
        signal(barrier, device)
    for o in range(1, row):
        signal(barrier, {"ba": my_y * row + ((me + o) & (row - 1))})
    loads = [
        pltpu.make_async_copy(x_hbm, x_ref, in_sem.at[0]),
        pltpu.make_async_copy(kb_hbm, kb_ref, in_sem.at[1]),
        pltpu.make_async_copy(gain_hbm, gain_ref, in_sem.at[2]),
        pltpu.make_async_copy(
            gt_hbm.at[:, pl.ds(pl.multiple_of(me * LANES, LANES), LANES)], recv.at[me], in_sem.at[3]),
    ]
    for load in loads:
        load.start()
    pl.semaphore_wait(barrier, row - 1 + 4)
    signal(ahead_sem.at[1], ahead(-1))
    signal(behind_sem.at[1], ahead(1))

    def bulk(r, dst):
        return pltpu.make_async_remote_copy(
            gt_hbm.at[:, pl.ds(pl.multiple_of(dst * LANES, LANES), LANES)],
            recv.at[me], send_sem, recv_sem.at[r],
            device_id={"ba": dst}, device_id_type=MESH)

    def send(r, _):
        to = at(*offset(r)) * NC
        bulk(r, to).start()
        bulk(r, to + 1).start()
        return 0

    bulk(CHIPS - 1, chip * NC + (1 - core)).start()
    first, heard = 0, [0, 0]
    for n_ahead, n_behind, offsets in STAGES:
        while heard[0] < n_ahead:
            heard[0] += 1
            pl.semaphore_wait(ahead_sem.at[heard[0]], 1)
            if heard[0] < NY // 2:
                signal(ahead_sem.at[heard[0] + 1], ahead(-1))
        while heard[1] < n_behind:
            heard[1] += 1
            pl.semaphore_wait(behind_sem.at[heard[1]], 1)
            if heard[1] < NY // 2 - 1:
                signal(behind_sem.at[heard[1] + 1], ahead(1))
        lax.fori_loop(first, first + len(offsets), send, 0)
        first += len(offsets)
    signal(above_sem.at[1], above(-1))
    signal(below_sem.at[1], above(1))

    lane = lax.broadcasted_iota(jnp.int32, (LANES, LANES), 1)
    word = lane >> 5
    shift = 31 - (lane & 31)
    for load in loads[:3]:
        load.wait()
    acc[...] = jnp.zeros_like(acc)

    def forward(k, _):
        x = x_ref[:, pl.ds(pl.multiple_of(k * LANES, LANES), LANES)].astype(jnp.float32)
        words = jnp.take_along_axis(kb_ref[...], word + 4 * k, axis=1)
        keep = jnp.where(jnp.left_shift(words, shift) < 0, 1.0, 0.0)
        dropped = x * keep * (1.0 / KEEP_RATE)
        keep_ref[k] = keep
        n_ref[k] = dropped
        acc[...] += dropped * dropped
        return 0

    lax.fori_loop(0, CHIPS, forward, 0)
    mean = jnp.sum(acc[...], axis=1, keepdims=True) * (1.0 / (CHIPS * LANES))
    inverse = lax.rsqrt(mean + EPSILON)

    def normalise(k, _):
        n_ref[k] = n_ref[k] * inverse
        return 0

    lax.fori_loop(0, CHIPS, normalise, 0)
    acc[...] = jnp.zeros_like(acc)

    def block(r, k):
        grads = recv[pl.ds(k * NC, NC)].reshape(LANES, LANES).astype(jnp.float32).T
        grads = grads * keep_ref[k]
        normed = n_ref[k]
        part[pl.ds(r, 1), :] = jnp.sum(grads * normed, axis=0, keepdims=True)
        scaled = grads * gain_ref[pl.ds(k, 1), :]
        gs_ref[k] = scaled
        acc[...] += scaled * normed

    def arrive(r, _):
        dy, dx = offset(r)
        k = at(-dy, -dx)
        both = recv.at[pl.ds(0, NC)]
        pltpu.make_async_copy(both, both, recv_sem.at[r]).wait()
        block(r, k)
        pltpu.make_async_remote_copy(
            part.at[pl.ds(r, 1)], ret.at[pl.ds(chip, 1)], psend_sem, pret_sem,
            device_id={"ba": k * NC + core}, device_id_type=MESH).start()
        return 0

    own = CHIPS - 1
    one = recv.at[0]
    pltpu.make_async_copy(one, one, recv_sem.at[own]).wait()
    loads[3].wait()
    block(own, chip)
    ret[pl.ds(chip, 1), :] = part[pl.ds(own, 1), :]
    reach = planes // 2
    steps = [len(ORDER) * (i + 1) // (reach + 2) for i in range(reach)]
    first = 0
    for i, until in enumerate(steps, 1):
        lax.fori_loop(first, until, arrive, 0)
        first = until
        pl.semaphore_wait(above_sem.at[i], 1)
        if i < reach:
            signal(above_sem.at[i + 1], above(-1))
        if i < planes - reach:
            pl.semaphore_wait(below_sem.at[i], 1)
            if i + 1 < planes - reach:
                signal(below_sem.at[i + 1], above(1))
    lax.fori_loop(first, len(ORDER), arrive, 0)

    centre = jnp.sum(acc[...], axis=1, keepdims=True) * (1.0 / (CHIPS * LANES))
    a = inverse * (1.0 / KEEP_RATE)
    b = a * centre

    def finish(k, _):
        gin_ref[:, pl.ds(pl.multiple_of(k * LANES, LANES), LANES)] = (a * gs_ref[k] - b * n_ref[k]).astype(jnp.bfloat16)
        return 0

    lax.fori_loop(0, CHIPS, finish, 0)

    rest = ret.at[pl.ds(0, CHIPS - 1)]
    pltpu.make_async_copy(rest, rest, pret_sem).wait()
    column[pl.ds(mine, 1), :] = jnp.sum(ret[...], axis=0, keepdims=True)

    def tell(o, _):
        p = lax.rem(mine + o, everyone)
        pltpu.make_async_remote_copy(
            column.at[pl.ds(mine, 1)], column.at[pl.ds(mine, 1)], csend_sem, crecv_sem,
            device_id={"aa": p >> 1, "ba": me - core + (p & 1)}, device_id_type=MESH).start()
        return 0

    lax.fori_loop(1, everyone, tell, 0)
    others = column.at[pl.ds(0, everyone - 1)]
    pltpu.make_async_copy(others, others, crecv_sem).wait()
    total = jnp.sum(column[...], axis=0, keepdims=True) * scale
    half = LANES // NC
    total_ref[...] = jnp.where(core == 0, total[:, :half], total[:, half:])
    pltpu.make_async_copy(rest, rest, psend_sem).wait()
    sent = recv.at[pl.ds(0, PEERS - 1)]
    pltpu.make_async_copy(sent, sent, send_sem).wait()
    pltpu.make_async_copy(others, others, csend_sem).wait()


def write_kernel(gin_ref, total_ref, gin_hbm, gain_hbm, sems):
    copies = [pltpu.make_async_copy(gin_ref, gin_hbm, sems.at[0]), pltpu.make_async_copy(total_ref, gain_hbm, sems.at[1])]
    for copy in copies:
        copy.start()
    for copy in copies:
        copy.wait()


def per_device(planes, grad_out, saved_input, keep_bits, gain):
    rows, width = saved_input.shape
    tokens = grad_out.shape[0] * planes
    vmem = functools.partial(pl.BlockSpec, memory_space=pltpu.VMEM)
    hbm = functools.partial(pl.BlockSpec, memory_space=pltpu.HBM)
    f32 = jnp.float32
    grad_in = jax.ShapeDtypeStruct((rows, width), jnp.bfloat16)
    share = jax.ShapeDtypeStruct((1, LANES // NC), f32)
    blocks = pltpu.VMEM((CHIPS, LANES, LANES), f32)
    results = pl.pallas_call(
        functools.partial(exchange_kernel, planes, 1.0 / math.sqrt(tokens)),
        name="exchange",
        out_shape=(pltpu.VMEM(grad_in.shape, grad_in.dtype), pltpu.VMEM(share.shape, f32)),
        in_specs=[hbm(), hbm(), hbm(), hbm()],
        out_specs=(vmem(), vmem()),
        scratch_shapes=[
            pltpu.VMEM((rows, width), jnp.bfloat16),
            pltpu.VMEM(keep_bits.shape, jnp.int32),
            pltpu.VMEM((CHIPS, LANES), f32),
            pltpu.VMEM((PEERS, LANES // NC, LANES), jnp.bfloat16),
            blocks, blocks, blocks,
            pltpu.VMEM((CHIPS, LANES), f32),
            pltpu.VMEM((CHIPS, LANES), f32),
            pltpu.VMEM((planes * NC, LANES), f32),
            pltpu.VMEM((LANES, LANES), f32),
            pltpu.SemaphoreType.DMA((4,)),
            pltpu.SemaphoreType.DMA,
            pltpu.SemaphoreType.DMA((CHIPS,)),
            pltpu.SemaphoreType.DMA,
            pltpu.SemaphoreType.DMA,
            pltpu.SemaphoreType.DMA,
            pltpu.SemaphoreType.DMA,
            pltpu.SemaphoreType.REGULAR((NY // 2 + 1,)),
            pltpu.SemaphoreType.REGULAR((NY // 2,)),
            pltpu.SemaphoreType.REGULAR((planes // 2 + 1,)),
            pltpu.SemaphoreType.REGULAR((planes - planes // 2,)),
        ],
        compiler_params=pltpu.CompilerParams(collective_id=0, has_side_effects=True, vmem_limit_bytes=24 << 20),
    )(*(pltpu.with_memory_space_constraint(a, pltpu.HBM) for a in (grad_out.T, saved_input, keep_bits, gain.reshape(CHIPS, LANES))))
    grad_in, share = pl.pallas_call(
        write_kernel,
        name="write",
        out_shape=(grad_in, share),
        in_specs=[vmem(), vmem()],
        out_specs=(hbm(), hbm()),
        scratch_shapes=[pltpu.SemaphoreType.DMA((2,))],
        compiler_params=pltpu.CompilerParams(vmem_limit_bytes=4 << 20),
    )(*results)
    return grad_in, share.reshape(LANES // NC)


def solution(mesh):
    placed = (P("aa", "ba"), P(("aa", "ba"), None), P(("aa", "ba"), None), P())
    return jax.shard_map(
        functools.partial(per_device, mesh.shape["aa"]),
        mesh=mesh,
        in_specs=placed,
        out_specs=(P(("aa", "ba"), None), P("ba")),
        check_vma=False,
    )
```

```python
import functools
import math

import jax
import jax.numpy as jnp
from jax import lax
from jax.experimental import pallas as pl
from jax.experimental.pallas import tpu as pltpu
from jax.sharding import PartitionSpec as P

KEEP_RATE = 0.9
EPSILON = 1e-06
MESH = pl.DeviceIdType.MESH
LANES = 128
NY, NX, NC = 8, 4, 2
CHIPS = NY * NX
PEERS = CHIPS * NC


FAR, NEAR = (4, 3, 5), (2, 6, 1, 7)
ORDER = (
    tuple((y, 0) for y in FAR)
    + ((0, 2), (0, 1), (0, 3))
    + tuple((y, 2) for y in FAR + NEAR)
    + tuple((y, 1) for y in FAR + NEAR)
    + tuple((y, 3) for y in FAR + NEAR)
    + tuple((y, 0) for y in NEAR)
)
HEAD = len(FAR)
LATE = 4
WINDOW = 31
PER_WORD = 6


def offset(r):
    codes = [dy * NX + dx for dy, dx in ORDER]
    words = [sum(c << (5 * i) for i, c in enumerate(codes[w:w + PER_WORD])) for w in range(0, len(codes), PER_WORD)]
    group = r // PER_WORD
    word = jnp.int32(words[0])
    for g, w in enumerate(words[1:], 1):
        word = jnp.where(group >= g, jnp.int32(w), word)
    code = (word >> (5 * (r - group * PER_WORD))) & (CHIPS - 1)
    return code >> 2, code & (NX - 1)


def exchange_kernel(
    planes, scale,
    gt_hbm, x_hbm, kb_hbm, gain_hbm, gin_ref, total_ref,
    x_ref, kb_ref, gain_ref, recv, keep_ref, n_ref, gs_ref, part, ret, column, acc,
    in_sem, send_sem, recv_sem, psend_sem, pret_sem, csend_sem, crecv_sem, row_sem, above_sem, below_sem,
):
    me = lax.axis_index("ba")
    plane = lax.axis_index("aa")
    core = me & 1
    chip = me >> 1
    my_y, my_x = chip >> 2, chip & (NX - 1)
    half = LANES // NC
    first_plane, last_plane = plane == 0, plane == planes - 1

    def at(dy, dx=0):
        return ((my_y + dy) & (NY - 1)) * NX + ((my_x + dx) & (NX - 1))

    def above(dz):
        return {"aa": lax.rem(plane + dz + planes, planes)}

    def signal(sem, device, inc=1):
        pl.semaphore_signal(sem, inc=inc, device_id=device, device_id_type=MESH)

    ret[...] = jnp.zeros_like(ret)
    barrier = pltpu.get_barrier_semaphore()
    for dy in (4, 3, 5, 2, 6, 1, 7):
        for c in range(NC):
            signal(barrier, {"ba": at(dy) * NC + c})
    for dx in (2, 1, 3):
        signal(barrier, {"ba": at(0, dx) * NC + core})
    signal(barrier, {"ba": me ^ 1})

    @pl.when(jnp.logical_not(last_plane))
    def _():
        signal(barrier, above(1))

    @pl.when(first_plane)
    def _():
        signal(barrier, above(-1))

    loads = [
        pltpu.make_async_copy(x_hbm, x_ref, in_sem.at[0]),
        pltpu.make_async_copy(kb_hbm, kb_ref, in_sem.at[1]),
        pltpu.make_async_copy(gain_hbm, gain_ref, in_sem.at[2]),
        pltpu.make_async_copy(
            gt_hbm.at[:, pl.ds(pl.multiple_of(me * LANES, LANES), LANES)], recv.at[me], in_sem.at[3]),
    ]
    for load in loads:
        load.start()
    near = (NY - 1) * NC + (NX - 1) + 1
    pl.semaphore_wait(barrier, jnp.where(first_plane, near, jnp.where(last_plane, near + 2, near + 1)))

    def bulk(r, dst):
        return pltpu.make_async_remote_copy(
            gt_hbm.at[:, pl.ds(pl.multiple_of(dst * LANES, LANES), LANES)],
            recv.at[me], send_sem, recv_sem.at[r],
            device_id={"ba": dst}, device_id_type=MESH)

    def send(r, _):
        to = at(*offset(r)) * NC
        bulk(r, to).start()
        bulk(r, to + 1).start()
        return 0

    for dx in (2, 1, 3):
        signal(row_sem.at[dx], {"ba": at(0, -dx) * NC + core})
    lax.fori_loop(0, HEAD, send, 0)
    bulk(CHIPS - 1, me ^ 1).start()
    for dx in (1, 3, 2):
        pl.semaphore_wait(row_sem.at[dx], 1)
    lax.fori_loop(HEAD, WINDOW, send, 0)

    @pl.when(jnp.logical_not(first_plane))
    def _():
        signal(above_sem.at[1], above(-1))

    @pl.when(last_plane)
    def _():
        signal(below_sem.at[1], above(1))

    lane = lax.broadcasted_iota(jnp.int32, (LANES, LANES), 1)
    word = lane >> 5
    shift = 31 - (lane & 31)
    for load in loads[:3]:
        load.wait()
    acc[...] = jnp.zeros_like(acc)

    def forward(k, _):
        x = x_ref[:, pl.ds(pl.multiple_of(k * LANES, LANES), LANES)].astype(jnp.float32)
        words = jnp.take_along_axis(kb_ref[...], word + 4 * k, axis=1)
        keep = jnp.where(jnp.left_shift(words, shift) < 0, 1.0, 0.0)
        dropped = x * keep * (1.0 / KEEP_RATE)
        keep_ref[k] = keep
        n_ref[k] = dropped
        acc[...] += dropped * dropped
        return 0

    lax.fori_loop(0, CHIPS, forward, 0)
    mean = jnp.sum(acc[...], axis=1, keepdims=True) * (1.0 / (CHIPS * LANES))
    inverse = lax.rsqrt(mean + EPSILON)

    def normalise(k, _):
        n_ref[k] = n_ref[k] * inverse
        return 0

    lax.fori_loop(0, CHIPS, normalise, 0)
    acc[...] = jnp.zeros_like(acc)

    def block(r, k):
        grads = recv[pl.ds(k * NC, NC)].reshape(LANES, LANES).astype(jnp.float32).T
        grads = grads * keep_ref[k]
        normed = n_ref[k]
        sums = jnp.sum(grads * normed, axis=0, keepdims=True)
        for c in range(NC):
            part[c, pl.ds(r, 1), :] = sums[:, c * half:(c + 1) * half]
        scaled = grads * gain_ref[pl.ds(k, 1), :]
        gs_ref[k] = scaled
        acc[...] += scaled * normed

    def give_back(r, owner, c):
        pltpu.make_async_remote_copy(
            part.at[c, pl.ds(r, 1)], ret.at[pl.ds(me, 1)], psend_sem, pret_sem,
            device_id={"ba": owner}, device_id_type=MESH).start()

    def await_block(r):
        dy, dx = offset(r)
        both = recv.at[pl.ds(0, NC)]
        pltpu.make_async_copy(both, both, recv_sem.at[r]).wait()
        k = at(-dy, -dx)
        block(r, k)
        return k

    def arrive(r, _):
        k = await_block(r)
        for c in range(NC):
            give_back(r, k * NC + c, c)
        if WINDOW < len(ORDER):
            @pl.when(r + WINDOW < len(ORDER))
            def _():
                send(r + WINDOW, 0)

        return 0

    early = len(ORDER) - LATE

    def arrive_late(r, _):
        k = await_block(r)
        slot = planes * (1 + (r - early) * NC + core) + plane
        for p in range(planes):
            for c in range(NC):
                pltpu.make_async_remote_copy(
                    part.at[c, pl.ds(r, 1)], column.at[pl.ds(slot, 1)], csend_sem, crecv_sem,
                    device_id={"aa": p, "ba": k * NC + c}, device_id_type=MESH).start()
        return 0

    own = CHIPS - 1
    one = recv.at[0]
    pltpu.make_async_copy(one, one, recv_sem.at[own]).wait()
    loads[3].wait()
    block(own, chip)

    @pl.when(core == 0)
    def _():
        give_back(own, me ^ 1, 1)
        ret[pl.ds(me, 1), :] = part[0, pl.ds(own, 1), :]

    @pl.when(core == 1)
    def _():
        give_back(own, me ^ 1, 0)
        ret[pl.ds(me, 1), :] = part[1, pl.ds(own, 1), :]

    reach = planes // 2
    steps = [early * (i + 1) // (reach + 2) for i in range(reach)]
    first = 0
    for i, until in enumerate(steps, 1):
        lax.fori_loop(first, until, arrive, 0)
        first = until
        pl.semaphore_wait(above_sem.at[i], 1)
        if i == 1:
            @pl.when(jnp.logical_not(last_plane))
            def _():
                signal(below_sem.at[1], above(1))

        if i < planes - reach:
            pl.semaphore_wait(below_sem.at[i], 1)
            if i == 1:
                @pl.when(first_plane)
                def _():
                    signal(above_sem.at[1], above(-1))

            if i + 1 < planes - reach:
                signal(below_sem.at[i + 1], above(1))
        if i < reach:
            signal(above_sem.at[i + 1], above(-1))
    lax.fori_loop(first, early, arrive, 0)
    lax.fori_loop(early, len(ORDER), arrive_late, 0)

    rest = ret.at[pl.ds(0, (CHIPS - LATE) * NC - 1)]
    pltpu.make_async_copy(rest, rest, pret_sem).wait()
    column[pl.ds(plane, 1), :] = jnp.sum(ret[...], axis=0, keepdims=True)

    def tell(o, _):
        pltpu.make_async_remote_copy(
            column.at[pl.ds(plane, 1)], column.at[pl.ds(plane, 1)], csend_sem, crecv_sem,
            device_id=above(o), device_id_type=MESH).start()
        return 0

    lax.fori_loop(1, planes, tell, 0)

    centre = jnp.sum(acc[...], axis=1, keepdims=True) * (1.0 / (CHIPS * LANES))
    a = inverse * (1.0 / KEEP_RATE)
    b = a * centre

    def finish(k, _):
        gin_ref[:, pl.ds(pl.multiple_of(k * LANES, LANES), LANES)] = (a * gs_ref[k] - b * n_ref[k]).astype(jnp.bfloat16)
        return 0

    lax.fori_loop(0, CHIPS, finish, 0)
    pltpu.make_async_copy(rest, rest, psend_sem).wait()
    sent = recv.at[pl.ds(0, PEERS - 1)]
    pltpu.make_async_copy(sent, sent, send_sem).wait()
    others = column.at[pl.ds(0, planes * (1 + LATE * NC) - 1)]
    pltpu.make_async_copy(others, others, csend_sem).wait()
    pltpu.make_async_copy(others, others, crecv_sem).wait()
    total_ref[...] = jnp.sum(column[...], axis=0, keepdims=True) * scale


def write_kernel(gin_ref, total_ref, gin_hbm, gain_hbm, sems):
    copies = [pltpu.make_async_copy(gin_ref, gin_hbm, sems.at[0]), pltpu.make_async_copy(total_ref, gain_hbm, sems.at[1])]
    for copy in copies:
        copy.start()
    for copy in copies:
        copy.wait()


def per_device(planes, grad_out, saved_input, keep_bits, gain):
    rows, width = saved_input.shape
    tokens = grad_out.shape[0] * planes
    vmem = functools.partial(pl.BlockSpec, memory_space=pltpu.VMEM)
    hbm = functools.partial(pl.BlockSpec, memory_space=pltpu.HBM)
    f32 = jnp.float32
    grad_in = jax.ShapeDtypeStruct((rows, width), jnp.bfloat16)
    share = jax.ShapeDtypeStruct((1, LANES // NC), f32)
    blocks = pltpu.VMEM((CHIPS, LANES, LANES), f32)
    results = pl.pallas_call(
        functools.partial(exchange_kernel, planes, 1.0 / math.sqrt(tokens)),
        name="exchange",
        out_shape=(pltpu.VMEM(grad_in.shape, grad_in.dtype), pltpu.VMEM(share.shape, f32)),
        in_specs=[hbm(), hbm(), hbm(), hbm()],
        out_specs=(vmem(), vmem()),
        scratch_shapes=[
            pltpu.VMEM((rows, width), jnp.bfloat16),
            pltpu.VMEM(keep_bits.shape, jnp.int32),
            pltpu.VMEM((CHIPS, LANES), f32),
            pltpu.VMEM((PEERS, LANES // NC, LANES), jnp.bfloat16),
            blocks, blocks, blocks,
            pltpu.VMEM((NC, CHIPS, LANES // NC), f32),
            pltpu.VMEM((PEERS, LANES // NC), f32),
            pltpu.VMEM((planes * (1 + LATE * NC), LANES // NC), f32),
            pltpu.VMEM((LANES, LANES), f32),
            pltpu.SemaphoreType.DMA((4,)),
            pltpu.SemaphoreType.DMA,
            pltpu.SemaphoreType.DMA((CHIPS,)),
            pltpu.SemaphoreType.DMA,
            pltpu.SemaphoreType.DMA,
            pltpu.SemaphoreType.DMA,
            pltpu.SemaphoreType.DMA,
            pltpu.SemaphoreType.REGULAR((NX,)),
            pltpu.SemaphoreType.REGULAR((planes // 2 + 1,)),
            pltpu.SemaphoreType.REGULAR((planes - planes // 2,)),
        ],
        compiler_params=pltpu.CompilerParams(collective_id=0, has_side_effects=True, vmem_limit_bytes=24 << 20),
    )(*(pltpu.with_memory_space_constraint(a, pltpu.HBM) for a in (grad_out.T, saved_input, keep_bits, gain.reshape(CHIPS, LANES))))
    grad_in, share = pl.pallas_call(
        write_kernel,
        name="write",
        out_shape=(grad_in, share),
        in_specs=[vmem(), vmem()],
        out_specs=(hbm(), hbm()),
        scratch_shapes=[pltpu.SemaphoreType.DMA((2,))],
        compiler_params=pltpu.CompilerParams(vmem_limit_bytes=4 << 20),
    )(*results)
    return grad_in, share.reshape(LANES // NC)


def solution(mesh):
    placed = (P("aa", "ba"), P(("aa", "ba"), None), P(("aa", "ba"), None), P())
    return jax.shard_map(
        functools.partial(per_device, mesh.shape["aa"]),
        mesh=mesh,
        in_specs=placed,
        out_specs=(P(("aa", "ba"), None), P("ba")),
        check_vma=False,
    )
```

```python
import functools
import math

import jax
import jax.numpy as jnp
from jax import lax
from jax.experimental import pallas as pl
from jax.experimental.pallas import tpu as pltpu
from jax.sharding import PartitionSpec as P

KEEP_RATE = 0.9
EPSILON = 1e-06
MESH = pl.DeviceIdType.MESH
LANES = 128
NY, NX, NC = 8, 4, 2
CHIPS = NY * NX
PEERS = CHIPS * NC


FAR, NEAR = (4, 3, 5), (2, 6, 1, 7)
ORDER = (
    tuple((y, 0) for y in FAR)
    + ((0, 2), (0, 1), (0, 3))
    + tuple((y, 2) for y in FAR + NEAR)
    + tuple((y, 1) for y in FAR + NEAR)
    + tuple((y, 3) for y in FAR + NEAR)
    + tuple((y, 0) for y in NEAR)
)
HEAD = len(FAR)
ADDER = 1
ADDING = 2
BOTH = 2 * NX
PER_WORD = 6


def offset(r):
    codes = [dy * NX + dx for dy, dx in ORDER]
    words = [sum(c << (5 * i) for i, c in enumerate(codes[w:w + PER_WORD])) for w in range(0, len(codes), PER_WORD)]
    group = r // PER_WORD
    word = jnp.int32(words[0])
    for g, w in enumerate(words[1:], 1):
        word = jnp.where(group >= g, jnp.int32(w), word)
    code = (word >> (5 * (r - group * PER_WORD))) & (CHIPS - 1)
    return code >> 2, code & (NX - 1)


def exchange_kernel(
    planes, scale,
    gt_hbm, x_hbm, kb_hbm, gain_hbm, gin_ref, total_ref,
    x_ref, kb_ref, gain_ref, recv, keep_ref, n_ref, gs_ref, part, rows, share, acc,
    in_sem, send_sem, recv_sem, rsend_sem, rrecv_sem, tsend_sem, trecv_sem, row_sem, up_sem, low_sem,
):
    me = lax.axis_index("ba")
    plane = lax.axis_index("aa")
    core = me & 1
    chip = me >> 1
    my_y, my_x = chip >> 2, chip & (NX - 1)
    half = LANES // NC
    first_plane, last_plane = plane == 0, plane == planes - 1
    alone = first_plane & (chip < BOTH)
    adds_up = (plane < ADDING) & (core == ADDER) | alone

    def at(dy, dx=0):
        return ((my_y + dy) & (NY - 1)) * NX + ((my_x + dx) & (NX - 1))

    def above(dz):
        return {"aa": lax.rem(plane + dz + planes, planes)}

    def signal(sem, device, inc=1):
        pl.semaphore_signal(sem, inc=inc, device_id=device, device_id_type=MESH)

    barrier = pltpu.get_barrier_semaphore()
    for dy in (4, 3, 5, 2, 6, 1, 7):
        for c in range(NC):
            signal(barrier, {"ba": at(dy) * NC + c})
    for dx in (2, 1, 3):
        signal(barrier, {"ba": at(0, dx) * NC + core})
    signal(barrier, {"ba": me ^ 1})

    @pl.when(jnp.logical_not(last_plane))
    def _():
        signal(barrier, above(1))

    loads = [
        pltpu.make_async_copy(x_hbm, x_ref, in_sem.at[0]),
        pltpu.make_async_copy(kb_hbm, kb_ref, in_sem.at[1]),
        pltpu.make_async_copy(gain_hbm, gain_ref, in_sem.at[2]),
        pltpu.make_async_copy(
            gt_hbm.at[:, pl.ds(pl.multiple_of(me * LANES, LANES), LANES)], recv.at[me], in_sem.at[3]),
    ]
    for load in loads:
        load.start()
    near = (NY - 1) * NC + (NX - 1) + 1
    pl.semaphore_wait(barrier, jnp.where(first_plane, near, jnp.where(last_plane, near + 2, near + 1)))

    def bulk(r, dst):
        return pltpu.make_async_remote_copy(
            gt_hbm.at[:, pl.ds(pl.multiple_of(dst * LANES, LANES), LANES)],
            recv.at[me], send_sem, recv_sem.at[r],
            device_id={"ba": dst}, device_id_type=MESH)

    def send(r, _):
        to = at(*offset(r)) * NC
        bulk(r, to).start()
        bulk(r, to + 1).start()
        return 0

    for dx in (2, 1, 3):
        signal(row_sem.at[dx], {"ba": at(0, -dx) * NC + core})
    lax.fori_loop(0, HEAD, send, 0)
    bulk(CHIPS - 1, me ^ 1).start()
    for dx in (1, 3, 2):
        pl.semaphore_wait(row_sem.at[dx], 1)
    lax.fori_loop(HEAD, len(ORDER), send, 0)

    homes = ADDING
    inner = jnp.logical_not(first_plane | last_plane)

    @pl.when(plane < homes - 1)
    def _():
        pl.semaphore_wait(up_sem, 1)

    @pl.when(inner)
    def _():
        signal(up_sem, above(-1))

    @pl.when(first_plane)
    def _():
        signal(low_sem, above(1))
        signal(barrier, above(-1))

    lane = lax.broadcasted_iota(jnp.int32, (LANES, LANES), 1)
    word = lane >> 5
    shift = 31 - (lane & 31)
    for load in loads[:3]:
        load.wait()
    acc[...] = jnp.zeros_like(acc)

    def forward(k, _):
        x = x_ref[:, pl.ds(pl.multiple_of(k * LANES, LANES), LANES)].astype(jnp.float32)
        words = jnp.take_along_axis(kb_ref[...], word + 4 * k, axis=1)
        keep = jnp.where(jnp.left_shift(words, shift) < 0, 1.0, 0.0)
        dropped = x * keep * (1.0 / KEEP_RATE)
        keep_ref[k] = keep
        n_ref[k] = dropped
        acc[...] += dropped * dropped
        return 0

    lax.fori_loop(0, CHIPS, forward, 0)
    mean = jnp.sum(acc[...], axis=1, keepdims=True) * (1.0 / (CHIPS * LANES))
    inverse = lax.rsqrt(mean + EPSILON)

    def normalise(k, _):
        n_ref[k] = n_ref[k] * inverse
        return 0

    lax.fori_loop(0, CHIPS, normalise, 0)
    acc[...] = jnp.zeros_like(acc)

    def block(r, k):
        grads = recv[pl.ds(k * NC, NC)].reshape(LANES, LANES).astype(jnp.float32).T
        grads = grads * keep_ref[k]
        normed = n_ref[k]
        part[pl.ds(r, 1), :] = jnp.sum(grads * normed, axis=0, keepdims=True)
        scaled = grads * gain_ref[pl.ds(k, 1), :]
        gs_ref[k] = scaled
        acc[...] += scaled * normed

    def give(r, device):
        pltpu.make_async_remote_copy(
            part.at[pl.ds(r, 1)], rows.at[pl.ds(plane * PEERS + me, 1)], rsend_sem, rrecv_sem,
            device_id=device, device_id_type=MESH).start()

    def give_back(r, k):
        for p in range(ADDING):
            give(r, {"aa": p, "ba": k * NC + ADDER})

        @pl.when(k < BOTH)
        def _():
            give(r, {"aa": 0, "ba": k * NC + 1 - ADDER})

    def arrive(r, _):
        dy, dx = offset(r)
        both = recv.at[pl.ds(0, NC)]
        pltpu.make_async_copy(both, both, recv_sem.at[r]).wait()
        k = at(-dy, -dx)
        block(r, k)
        give_back(r, k)
        return 0

    @pl.when((plane >= homes - 1) & (plane < planes - 2))
    def _():
        pl.semaphore_wait(up_sem, 1)

    @pl.when(inner)
    def _():
        pl.semaphore_wait(low_sem, 1)

    @pl.when(inner & (plane < planes - 2))
    def _():
        signal(low_sem, above(1))

    own = CHIPS - 1
    one = recv.at[0]
    pltpu.make_async_copy(one, one, recv_sem.at[own]).wait()
    loads[3].wait()
    block(own, chip)

    @pl.when(adds_up)
    def _():
        rows[pl.ds(plane * PEERS + me, 1), :] = part[pl.ds(own, 1), :]

    for p, c in [(p, ADDER) for p in range(ADDING)] + [(0, 1 - ADDER)]:
        there = jnp.logical_not((plane == p) & (core == c))
        if c != ADDER:
            there = there & (chip < BOTH)

        @pl.when(there)
        def _():
            give(own, {"aa": p, "ba": chip * NC + c})

    lax.fori_loop(0, len(ORDER), arrive, 0)

    centre = jnp.sum(acc[...], axis=1, keepdims=True) * (1.0 / (CHIPS * LANES))
    a = inverse * (1.0 / KEEP_RATE)
    b = a * centre

    def finish(k, _):
        gin_ref[:, pl.ds(pl.multiple_of(k * LANES, LANES), LANES)] = (a * gs_ref[k] - b * n_ref[k]).astype(jnp.bfloat16)
        return 0

    lax.fori_loop(0, CHIPS, finish, 0)
    sent = recv.at[pl.ds(0, PEERS - 1)]
    pltpu.make_async_copy(sent, sent, send_sem).wait()

    teller = plane == ADDING - 1

    def tell(device):
        pltpu.make_async_remote_copy(
            share, share, tsend_sem, trecv_sem, device_id=device, device_id_type=MESH).start()

    @pl.when(adds_up)
    def _():
        others = rows.at[pl.ds(0, planes * PEERS - 1)]
        pltpu.make_async_copy(others, others, rrecv_sem).wait()
        share[...] = jnp.sum(rows[...], axis=0, keepdims=True) * scale

        @pl.when(jnp.logical_not(alone))
        def _():
            tell({"ba": me ^ 1})

        @pl.when(teller)
        def _():
            def tell_plane(p, _):
                for c in range(NC):
                    tell({"aa": p, "ba": chip * NC + c})
                return 0

            lax.fori_loop(ADDING, planes, tell_plane, 0)

            told = rows.at[pl.ds(0, (planes - ADDING) * NC)]
            pltpu.make_async_copy(told, told, tsend_sem).wait()

        @pl.when(jnp.logical_not(alone))
        def _():
            pltpu.make_async_copy(share, share, tsend_sem).wait()

        given = rows.at[pl.ds(0, ADDING * CHIPS + BOTH - 1)]
        pltpu.make_async_copy(given, given, rsend_sem).wait()

    @pl.when(jnp.logical_not(adds_up))
    def _():
        given = rows.at[pl.ds(0, ADDING * CHIPS + BOTH)]
        pltpu.make_async_copy(given, given, rsend_sem).wait()
        pltpu.make_async_copy(share, share, trecv_sem).wait()

    total_ref[...] = jnp.where(core == 0, share[:, :half], share[:, half:])


def write_kernel(gin_ref, total_ref, gin_hbm, gain_hbm, sems):
    copies = [pltpu.make_async_copy(gin_ref, gin_hbm, sems.at[0]), pltpu.make_async_copy(total_ref, gain_hbm, sems.at[1])]
    for copy in copies:
        copy.start()
    for copy in copies:
        copy.wait()


def per_device(planes, grad_out, saved_input, keep_bits, gain):
    rows, width = saved_input.shape
    tokens = grad_out.shape[0] * planes
    vmem = functools.partial(pl.BlockSpec, memory_space=pltpu.VMEM)
    hbm = functools.partial(pl.BlockSpec, memory_space=pltpu.HBM)
    f32 = jnp.float32
    grad_in = jax.ShapeDtypeStruct((rows, width), jnp.bfloat16)
    share = jax.ShapeDtypeStruct((1, LANES // NC), f32)
    blocks = pltpu.VMEM((CHIPS, LANES, LANES), f32)
    results = pl.pallas_call(
        functools.partial(exchange_kernel, planes, 1.0 / math.sqrt(tokens)),
        name="exchange",
        out_shape=(pltpu.VMEM(grad_in.shape, grad_in.dtype), pltpu.VMEM(share.shape, f32)),
        in_specs=[hbm(), hbm(), hbm(), hbm()],
        out_specs=(vmem(), vmem()),
        scratch_shapes=[
            pltpu.VMEM((rows, width), jnp.bfloat16),
            pltpu.VMEM(keep_bits.shape, jnp.int32),
            pltpu.VMEM((CHIPS, LANES), f32),
            pltpu.VMEM((PEERS, LANES // NC, LANES), jnp.bfloat16),
            blocks, blocks, blocks,
            pltpu.VMEM((CHIPS, LANES), f32),
            pltpu.VMEM((planes * PEERS, LANES), f32),
            pltpu.VMEM((1, LANES), f32),
            pltpu.VMEM((LANES, LANES), f32),
            pltpu.SemaphoreType.DMA((4,)),
            pltpu.SemaphoreType.DMA,
            pltpu.SemaphoreType.DMA((CHIPS,)),
            pltpu.SemaphoreType.DMA,
            pltpu.SemaphoreType.DMA,
            pltpu.SemaphoreType.DMA,
            pltpu.SemaphoreType.DMA,
            pltpu.SemaphoreType.REGULAR((NX,)),
            pltpu.SemaphoreType.REGULAR,
            pltpu.SemaphoreType.REGULAR,
        ],
        compiler_params=pltpu.CompilerParams(collective_id=0, has_side_effects=True, vmem_limit_bytes=24 << 20),
    )(*(pltpu.with_memory_space_constraint(a, pltpu.HBM) for a in (grad_out.T, saved_input, keep_bits, gain.reshape(CHIPS, LANES))))
    grad_in, share = pl.pallas_call(
        write_kernel,
        name="write",
        out_shape=(grad_in, share),
        in_specs=[vmem(), vmem()],
        out_specs=(hbm(), hbm()),
        scratch_shapes=[pltpu.SemaphoreType.DMA((2,))],
        compiler_params=pltpu.CompilerParams(vmem_limit_bytes=4 << 20),
    )(*results)
    return grad_in, share.reshape(LANES // NC)


def solution(mesh):
    placed = (P("aa", "ba"), P(("aa", "ba"), None), P(("aa", "ba"), None), P())
    return jax.shard_map(
        functools.partial(per_device, mesh.shape["aa"]),
        mesh=mesh,
        in_specs=placed,
        out_specs=(P(("aa", "ba"), None), P("ba")),
        check_vma=False,
    )
```

```python
import functools
import math

import jax
import jax.numpy as jnp
from jax import lax
from jax.experimental import pallas as pl
from jax.experimental.pallas import tpu as pltpu
from jax.sharding import PartitionSpec as P

KEEP_RATE = 0.9
EPSILON = 1e-06
MESH = pl.DeviceIdType.MESH
LANES = 128
NY, NX, NC = 8, 4, 2
CHIPS = NY * NX
PEERS = CHIPS * NC


FAR, NEAR = (4, 3, 5), (2, 6, 1, 7)
ORDER = (
    tuple((y, 0) for y in FAR)
    + ((0, 2), (0, 1), (0, 3))
    + tuple((y, 2) for y in FAR + NEAR)
    + tuple((y, 1) for y in FAR + NEAR)
    + tuple((y, 3) for y in FAR + NEAR)
    + tuple((y, 0) for y in NEAR)
)
HEAD = len(FAR)
ADDER = 1
FIRST = 2 * NX
GROUPS = (6, 13, 20)
SEMAPHORES = len(GROUPS) + len(ORDER) - GROUPS[-1] + 1
PER_WORD = 6


def offset(r):
    codes = [dy * NX + dx for dy, dx in ORDER]
    words = [sum(c << (5 * i) for i, c in enumerate(codes[w:w + PER_WORD])) for w in range(0, len(codes), PER_WORD)]
    group = r // PER_WORD
    word = jnp.int32(words[0])
    for g, w in enumerate(words[1:], 1):
        word = jnp.where(group >= g, jnp.int32(w), word)
    code = (word >> (5 * (r - group * PER_WORD))) & (CHIPS - 1)
    return code >> 2, code & (NX - 1)


def exchange_kernel(
    planes, scale,
    gt_hbm, x_hbm, kb_hbm, gain_hbm, gin_ref, total_ref,
    gt_ref, x_ref, kb_ref, gain_ref, recv, keep_ref, n_ref, gs_ref, part, rows, share, acc,
    in_sem, send_sem, recv_sem, rsend_sem, rrecv_sem, tsend_sem, trecv_sem, row_sem, up_sem, low_sem,
):
    me = lax.axis_index("ba")
    plane = lax.axis_index("aa")
    core = me & 1
    chip = me >> 1
    my_y, my_x = chip >> 2, chip & (NX - 1)
    half = LANES // NC
    first_plane, last_plane = plane == 0, plane == planes - 1
    adder, first_chips = core == ADDER, chip < FIRST
    alone = first_plane & first_chips
    tells = adder & (first_plane & jnp.logical_not(first_chips) | (plane == 1) & first_chips)
    adds_up = alone | tells

    def at(dy, dx=0):
        return ((my_y + dy) & (NY - 1)) * NX + ((my_x + dx) & (NX - 1))

    def above(dz):
        return {"aa": lax.rem(plane + dz + planes, planes)}

    def signal(sem, device, inc=1):
        pl.semaphore_signal(sem, inc=inc, device_id=device, device_id_type=MESH)

    barrier = pltpu.get_barrier_semaphore()
    for dy in (4, 3, 5, 2, 6, 1, 7):
        for c in range(NC):
            signal(barrier, {"ba": at(dy) * NC + c})
    for dx in (2, 1, 3):
        signal(barrier, {"ba": at(0, dx) * NC + core})
    signal(barrier, {"ba": me ^ 1})

    @pl.when(jnp.logical_not(last_plane))
    def _():
        signal(barrier, above(1))

    loads = [
        pltpu.make_async_copy(source, target, in_sem.at[i])
        for i, (source, target) in enumerate(((gt_hbm, gt_ref), (x_hbm, x_ref), (kb_hbm, kb_ref), (gain_hbm, gain_ref)))
    ]
    for load in loads:
        load.start()
    near = (NY - 1) * NC + (NX - 1) + 1
    loads[0].wait()
    pl.semaphore_wait(barrier, jnp.where(first_plane, near, jnp.where(last_plane, near + 2, near + 1)))

    def bulk(dst, sem):
        pltpu.make_async_remote_copy(
            gt_ref.at[:, pl.ds(pl.multiple_of(dst * LANES, LANES), LANES)],
            recv.at[me], send_sem, recv_sem.at[sem],
            device_id={"ba": dst}, device_id_type=MESH).start()

    def serve(first, end, sem):
        def send(r, _):
            to = at(*offset(r)) * NC
            for c in range(NC):
                bulk(to + c, sem(r))
            return 0

        lax.fori_loop(first, end, send, 0)

    def single(r):
        return r - GROUPS[-1] + len(GROUPS)

    own_sem = SEMAPHORES - 1

    for dx in (2, 1, 3):
        signal(row_sem.at[dx - 1], {"ba": at(0, -dx) * NC + core})
    serve(0, HEAD, lambda r: 0)
    bulk(me ^ 1, own_sem)
    for dx in (1, 3, 2):
        pl.semaphore_wait(row_sem.at[dx - 1], 1)
    first = HEAD
    for g, end in enumerate(GROUPS):
        serve(first, end, lambda r: g)
        first = end
    serve(first, len(ORDER), single)

    homes = 2
    inner = jnp.logical_not(first_plane | last_plane)

    @pl.when(plane < homes - 1)
    def _():
        pl.semaphore_wait(up_sem, 1)

    @pl.when(inner)
    def _():
        signal(up_sem, above(-1))

    @pl.when(first_plane)
    def _():
        signal(low_sem, above(1))
        signal(barrier, above(-1))

    lane = lax.broadcasted_iota(jnp.int32, (LANES, LANES), 1)
    word = lane >> 5
    shift = 31 - (lane & 31)
    for load in loads[1:]:
        load.wait()
    recv[me] = gt_ref[:, pl.ds(pl.multiple_of(me * LANES, LANES), LANES)]
    acc[...] = jnp.zeros_like(acc)

    def forward(k, _):
        x = x_ref[:, pl.ds(pl.multiple_of(k * LANES, LANES), LANES)].astype(jnp.float32)
        words = jnp.take_along_axis(kb_ref[...], word + 4 * k, axis=1)
        keep = jnp.where(jnp.left_shift(words, shift) < 0, 1.0, 0.0)
        dropped = x * keep * (1.0 / KEEP_RATE)
        keep_ref[k] = keep
        n_ref[k] = dropped
        acc[...] += dropped * dropped
        return 0

    lax.fori_loop(0, CHIPS, forward, 0)
    mean = jnp.sum(acc[...], axis=1, keepdims=True) * (1.0 / (CHIPS * LANES))
    inverse = lax.rsqrt(mean + EPSILON)

    def normalise(k, _):
        n_ref[k] = n_ref[k] * inverse
        return 0

    lax.fori_loop(0, CHIPS, normalise, 0)
    acc[...] = jnp.zeros_like(acc)

    def block(r, k):
        grads = recv[pl.ds(k * NC, NC)].reshape(LANES, LANES).astype(jnp.float32).T
        grads = grads * keep_ref[k]
        normed = n_ref[k]
        part[pl.ds(r, 1), :] = jnp.sum(grads * normed, axis=0, keepdims=True)
        scaled = grads * gain_ref[pl.ds(k, 1), :]
        gs_ref[k] = scaled
        acc[...] += scaled * normed

    def give(r, device):
        pltpu.make_async_remote_copy(
            part.at[pl.ds(r, 1)], rows.at[pl.ds(plane * PEERS + me, 1)], rsend_sem, rrecv_sem,
            device_id=device, device_id_type=MESH).start()

    def give_back(r, k):
        give(r, {"aa": 0, "ba": k * NC + ADDER})

        @pl.when(k < FIRST)
        def _():
            give(r, {"aa": 1, "ba": k * NC + ADDER})
            give(r, {"aa": 0, "ba": k * NC + 1 - ADDER})

    def await_blocks(chips, sem):
        blocks = recv.at[pl.ds(0, chips * NC)]
        pltpu.make_async_copy(blocks, blocks, recv_sem.at[sem]).wait()

    def use(r, _):
        dy, dx = offset(r)
        k = at(-dy, -dx)
        block(r, k)
        give_back(r, k)
        return 0

    def arrive(r, _):
        await_blocks(1, single(r))
        return use(r, 0)

    @pl.when((plane >= homes - 1) & (plane < planes - 2))
    def _():
        pl.semaphore_wait(up_sem, 1)

    @pl.when(inner)
    def _():
        pl.semaphore_wait(low_sem, 1)

    @pl.when(inner & (plane < planes - 2))
    def _():
        signal(low_sem, above(1))

    own = CHIPS - 1
    one = recv.at[0]
    pltpu.make_async_copy(one, one, recv_sem.at[own_sem]).wait()
    block(own, chip)

    @pl.when(adds_up)
    def _():
        rows[pl.ds(plane * PEERS + me, 1), :] = part[pl.ds(own, 1), :]

    for p, c in ((0, ADDER), (1, ADDER), (0, 1 - ADDER)):
        there = jnp.logical_not((plane == p) & (core == c))
        if (p, c) != (0, ADDER):
            there = there & first_chips

        @pl.when(there)
        def _():
            give(own, {"aa": p, "ba": chip * NC + c})

    first = 0
    for g, end in enumerate(GROUPS):
        await_blocks(end - first, g)
        lax.fori_loop(first, end, use, 0)
        first = end
    lax.fori_loop(first, len(ORDER), arrive, 0)

    centre = jnp.sum(acc[...], axis=1, keepdims=True) * (1.0 / (CHIPS * LANES))
    a = inverse * (1.0 / KEEP_RATE)
    b = a * centre

    def finish(k, _):
        gin_ref[:, pl.ds(pl.multiple_of(k * LANES, LANES), LANES)] = (a * gs_ref[k] - b * n_ref[k]).astype(jnp.bfloat16)
        return 0

    lax.fori_loop(0, CHIPS, finish, 0)
    sent = recv.at[pl.ds(0, PEERS - 1)]
    pltpu.make_async_copy(sent, sent, send_sem).wait()

    def tell(device):
        pltpu.make_async_remote_copy(
            share, share, tsend_sem, trecv_sem, device_id=device, device_id_type=MESH).start()

    def tell_plane(p, _):
        for c in (ADDER, 1 - ADDER):
            tell({"aa": p, "ba": chip * NC + c})
        return 0

    count = CHIPS + 2 * FIRST

    @pl.when(adds_up)
    def _():
        others = rows.at[pl.ds(0, planes * PEERS - 1)]
        pltpu.make_async_copy(others, others, rrecv_sem).wait()
        share[...] = jnp.sum(rows[...], axis=0, keepdims=True) * scale

        @pl.when(tells)
        def _():
            tell({"ba": me ^ 1})

        @pl.when(tells & first_plane)
        def _():
            lax.fori_loop(1, planes, tell_plane, 0)
            told = rows.at[pl.ds(0, planes * NC - 1)]
            pltpu.make_async_copy(told, told, tsend_sem).wait()

        @pl.when(tells & jnp.logical_not(first_plane))
        def _():
            lax.fori_loop(2, planes, tell_plane, 0)
            told = rows.at[pl.ds(0, (planes - 1) * NC - 1)]
            pltpu.make_async_copy(told, told, tsend_sem).wait()

        given = rows.at[pl.ds(0, count - 1)]
        pltpu.make_async_copy(given, given, rsend_sem).wait()

    @pl.when(jnp.logical_not(adds_up))
    def _():
        given = rows.at[pl.ds(0, count)]
        pltpu.make_async_copy(given, given, rsend_sem).wait()
        pltpu.make_async_copy(share, share, trecv_sem).wait()

    total_ref[...] = jnp.where(core == 0, share[:, :half], share[:, half:])


def write_kernel(gin_ref, total_ref, gin_hbm, gain_hbm, sems):
    copies = [pltpu.make_async_copy(gin_ref, gin_hbm, sems.at[0]), pltpu.make_async_copy(total_ref, gain_hbm, sems.at[1])]
    for copy in copies:
        copy.start()
    for copy in copies:
        copy.wait()


def per_device(planes, grad_out, saved_input, keep_bits, gain):
    rows, width = saved_input.shape
    tokens = grad_out.shape[0] * planes
    vmem = functools.partial(pl.BlockSpec, memory_space=pltpu.VMEM)
    hbm = functools.partial(pl.BlockSpec, memory_space=pltpu.HBM)
    f32 = jnp.float32
    grad_in = jax.ShapeDtypeStruct((rows, width), jnp.bfloat16)
    share = jax.ShapeDtypeStruct((1, LANES // NC), f32)
    blocks = pltpu.VMEM((CHIPS, LANES, LANES), f32)
    results = pl.pallas_call(
        functools.partial(exchange_kernel, planes, 1.0 / math.sqrt(tokens)),
        name="exchange",
        out_shape=(pltpu.VMEM(grad_in.shape, grad_in.dtype), pltpu.VMEM(share.shape, f32)),
        in_specs=[hbm(), hbm(), hbm(), hbm()],
        out_specs=(vmem(), vmem()),
        scratch_shapes=[
            pltpu.VMEM((LANES // NC, PEERS * LANES), jnp.bfloat16),
            pltpu.VMEM((rows, width), jnp.bfloat16),
            pltpu.VMEM(keep_bits.shape, jnp.int32),
            pltpu.VMEM((CHIPS, LANES), f32),
            pltpu.VMEM((PEERS, LANES // NC, LANES), jnp.bfloat16),
            blocks, blocks, blocks,
            pltpu.VMEM((CHIPS, LANES), f32),
            pltpu.VMEM((planes * PEERS, LANES), f32),
            pltpu.VMEM((1, LANES), f32),
            pltpu.VMEM((LANES, LANES), f32),
            pltpu.SemaphoreType.DMA((4,)),
            pltpu.SemaphoreType.DMA,
            pltpu.SemaphoreType.DMA((SEMAPHORES,)),
            pltpu.SemaphoreType.DMA,
            pltpu.SemaphoreType.DMA,
            pltpu.SemaphoreType.DMA,
            pltpu.SemaphoreType.DMA,
            pltpu.SemaphoreType.REGULAR((NX - 1,)),
            pltpu.SemaphoreType.REGULAR,
            pltpu.SemaphoreType.REGULAR,
        ],
        compiler_params=pltpu.CompilerParams(collective_id=0, has_side_effects=True, vmem_limit_bytes=24 << 20),
    )(*(pltpu.with_memory_space_constraint(a, pltpu.HBM) for a in (grad_out.T, saved_input, keep_bits, gain.reshape(CHIPS, LANES))))
    grad_in, share = pl.pallas_call(
        write_kernel,
        name="write",
        out_shape=(grad_in, share),
        in_specs=[vmem(), vmem()],
        out_specs=(hbm(), hbm()),
        scratch_shapes=[pltpu.SemaphoreType.DMA((2,))],
        compiler_params=pltpu.CompilerParams(vmem_limit_bytes=4 << 20),
    )(*results)
    return grad_in, share.reshape(LANES // NC)


def solution(mesh):
    placed = (P("aa", "ba"), P(("aa", "ba"), None), P(("aa", "ba"), None), P())
    return jax.shard_map(
        functools.partial(per_device, mesh.shape["aa"]),
        mesh=mesh,
        in_specs=placed,
        out_specs=(P(("aa", "ba"), None), P("ba")),
        check_vma=False,
    )
```

```python
import functools
import math

import jax
import jax.numpy as jnp
from jax import lax
from jax.experimental import pallas as pl
from jax.experimental.pallas import tpu as pltpu
from jax.sharding import PartitionSpec as P

KEEP_RATE = 0.9
EPSILON = 1e-06
MESH = pl.DeviceIdType.MESH
LANES = 128
NY, NX, NC = 8, 4, 2
CHIPS = NY * NX
PEERS = CHIPS * NC


FAR, NEAR = (4, 3, 5), (2, 6, 1, 7)
ORDER = (
    tuple((y, 0) for y in FAR)
    + ((0, 2), (0, 1), (0, 3))
    + tuple((y, 2) for y in FAR + NEAR)
    + tuple((y, 1) for y in FAR + NEAR)
    + tuple((y, 3) for y in FAR + NEAR)
    + tuple((y, 0) for y in NEAR)
)
HEAD = len(FAR)
ADDER = 1
FIRST = 2 * NX
GROUPS = (6, 13, 20)
SEMAPHORES = len(GROUPS) + len(ORDER) - GROUPS[-1] + 1
DETOUR = 20
DETOURS = ((7, 3, 0), (6, 2, 0))
PASS_AFTER = (6, 13, 20)
DETOUR_USE = 21
PER_WORD = 6


def offset(r):
    codes = [dy * NX + dx for dy, dx in ORDER]
    words = [sum(c << (5 * i) for i, c in enumerate(codes[w:w + PER_WORD])) for w in range(0, len(codes), PER_WORD)]
    group = r // PER_WORD
    word = jnp.int32(words[0])
    for g, w in enumerate(words[1:], 1):
        word = jnp.where(group >= g, jnp.int32(w), word)
    code = (word >> (5 * (r - group * PER_WORD))) & (CHIPS - 1)
    return code >> 2, code & (NX - 1)


def exchange_kernel(
    planes, scale,
    gt_hbm, x_hbm, kb_hbm, gain_hbm, gin_ref, total_ref,
    gt_ref, x_ref, kb_ref, gain_ref, recv, keep_ref, n_ref, gs_ref, part, rows, share, acc, relay,
    in_sem, send_sem, recv_sem, rsend_sem, rrecv_sem, tsend_sem, trecv_sem, row_sem, up_sem, low_sem, relay_sem, fsend_sem,
):
    me = lax.axis_index("ba")
    plane = lax.axis_index("aa")
    core = me & 1
    chip = me >> 1
    my_y, my_x = chip >> 2, chip & (NX - 1)
    half = LANES // NC
    first_plane, last_plane = plane == 0, plane == planes - 1
    adder, first_chips = core == ADDER, chip < FIRST
    alone = first_plane & first_chips
    tells = adder & (first_plane & jnp.logical_not(first_chips) | (plane == 1) & first_chips)
    adds_up = alone | tells

    def at(dy, dx=0):
        return ((my_y + dy) & (NY - 1)) * NX + ((my_x + dx) & (NX - 1))

    def above(dz):
        return {"aa": lax.rem(plane + dz + planes, planes)}

    def signal(sem, device, inc=1):
        pl.semaphore_signal(sem, inc=inc, device_id=device, device_id_type=MESH)

    barrier = pltpu.get_barrier_semaphore()
    for dy in (4, 3, 5, 2, 6, 1, 7):
        for c in range(NC):
            signal(barrier, {"ba": at(dy) * NC + c})
    for dx in (2, 1, 3):
        signal(barrier, {"ba": at(0, dx) * NC + core})
    signal(barrier, {"ba": me ^ 1})

    @pl.when(jnp.logical_not(last_plane))
    def _():
        signal(barrier, above(1))

    loads = [
        pltpu.make_async_copy(source, target, in_sem.at[i])
        for i, (source, target) in enumerate(((gt_hbm, gt_ref), (x_hbm, x_ref), (kb_hbm, kb_ref), (gain_hbm, gain_ref)))
    ]
    for load in loads:
        load.start()
    near = (NY - 1) * NC + (NX - 1) + 1
    loads[0].wait()
    pl.semaphore_wait(barrier, jnp.where(first_plane, near, jnp.where(last_plane, near + 2, near + 1)))

    def bulk(dst, sem):
        pltpu.make_async_remote_copy(
            gt_ref.at[:, pl.ds(pl.multiple_of(dst * LANES, LANES), LANES)],
            recv.at[me], send_sem, recv_sem.at[sem],
            device_id={"ba": dst}, device_id_type=MESH).start()

    def serve(first, end, sem):
        def send(r, _):
            to = at(*offset(r)) * NC
            for c in range(NC):
                bulk(to + c, sem(r))
            return 0

        lax.fori_loop(first, end, send, 0)

    def single(r):
        return r - GROUPS[-1] + len(GROUPS)

    own_sem = SEMAPHORES - 1

    for dx in (2, 1, 3):
        signal(row_sem.at[dx - 1], {"ba": at(0, -dx) * NC + core})
    serve(0, HEAD, lambda r: 0)
    bulk(me ^ 1, own_sem)
    for dx in (1, 3, 2):
        pl.semaphore_wait(row_sem.at[dx - 1], 1)
    first = HEAD
    for g, end in enumerate(GROUPS):
        serve(first, end, lambda r: g)
        first = end
    slots = max(s for _, _, s in DETOURS) + 1
    detours, via_plane, my_slot = False, plane, 0
    for late, via, slot in DETOURS:
        detours = detours | (plane == late)
        via_plane = jnp.where(plane == late, via, via_plane)
        my_slot = jnp.where(plane == late, slot, my_slot)
    serve(first, DETOUR, single)

    @pl.when(jnp.logical_not(detours))
    def _():
        serve(DETOUR, DETOUR + 1, single)

    serve(DETOUR + 1, len(ORDER), single)

    homes = 2
    inner = jnp.logical_not(first_plane | last_plane)

    @pl.when(plane < homes - 1)
    def _():
        pl.semaphore_wait(up_sem, 1)

    @pl.when(inner)
    def _():
        signal(up_sem, above(-1))

    @pl.when(first_plane)
    def _():
        signal(low_sem, above(1))
        signal(barrier, above(-1))

    lane = lax.broadcasted_iota(jnp.int32, (LANES, LANES), 1)
    word = lane >> 5
    shift = 31 - (lane & 31)
    for load in loads[1:]:
        load.wait()
    recv[me] = gt_ref[:, pl.ds(pl.multiple_of(me * LANES, LANES), LANES)]
    acc[...] = jnp.zeros_like(acc)

    def forward(k, _):
        x = x_ref[:, pl.ds(pl.multiple_of(k * LANES, LANES), LANES)].astype(jnp.float32)
        words = jnp.take_along_axis(kb_ref[...], word + 4 * k, axis=1)
        keep = jnp.where(jnp.left_shift(words, shift) < 0, 1.0, 0.0)
        dropped = x * keep * (1.0 / KEEP_RATE)
        keep_ref[k] = keep
        n_ref[k] = dropped
        acc[...] += dropped * dropped
        return 0

    lax.fori_loop(0, CHIPS, forward, 0)
    mean = jnp.sum(acc[...], axis=1, keepdims=True) * (1.0 / (CHIPS * LANES))
    inverse = lax.rsqrt(mean + EPSILON)

    def normalise(k, _):
        n_ref[k] = n_ref[k] * inverse
        return 0

    lax.fori_loop(0, CHIPS, normalise, 0)
    acc[...] = jnp.zeros_like(acc)

    def block(r, k):
        grads = recv[pl.ds(k * NC, NC)].reshape(LANES, LANES).astype(jnp.float32).T
        grads = grads * keep_ref[k]
        normed = n_ref[k]
        part[pl.ds(r, 1), :] = jnp.sum(grads * normed, axis=0, keepdims=True)
        scaled = grads * gain_ref[pl.ds(k, 1), :]
        gs_ref[k] = scaled
        acc[...] += scaled * normed

    def give(r, device):
        pltpu.make_async_remote_copy(
            part.at[pl.ds(r, 1)], rows.at[pl.ds(plane * PEERS + me, 1)], rsend_sem, rrecv_sem,
            device_id=device, device_id_type=MESH).start()

    def give_back(r, k):
        give(r, {"aa": 0, "ba": k * NC + ADDER})

        @pl.when(k < FIRST)
        def _():
            give(r, {"aa": 1, "ba": k * NC + ADDER})
            give(r, {"aa": 0, "ba": k * NC + 1 - ADDER})

    def await_blocks(chips, sem):
        blocks = recv.at[pl.ds(0, chips * NC)]
        pltpu.make_async_copy(blocks, blocks, recv_sem.at[sem]).wait()

    def use(r, _):
        dy, dx = offset(r)
        k = at(-dy, -dx)
        block(r, k)
        give_back(r, k)
        return 0

    def arrive(r, _):
        await_blocks(1, single(r))
        return use(r, 0)

    @pl.when((plane >= homes - 1) & (plane < planes - 2))
    def _():
        pl.semaphore_wait(up_sem, 1)

    @pl.when(inner)
    def _():
        pl.semaphore_wait(low_sem, 1)

    @pl.when(inner & (plane < planes - 2))
    def _():
        signal(low_sem, above(1))

    dy, dx = ORDER[DETOUR]

    @pl.when(detours)
    def _():
        to = at(dy, dx) * NC
        for c in range(NC):
            pltpu.make_async_remote_copy(
                gt_ref.at[:, pl.ds(pl.multiple_of((to + c) * LANES, LANES), LANES)],
                relay.at[my_slot * NC + core], send_sem, relay_sem.at[my_slot],
                device_id={"aa": via_plane, "ba": to + c}, device_id_type=MESH).start()

    def pass_on(slot):
        passes, to_plane = False, plane
        for late, via, there in DETOURS:
            if there == slot:
                passes = passes | (plane == via)
                to_plane = jnp.where(plane == via, late, to_plane)

        @pl.when(passes)
        def _():
            blocks = relay.at[pl.ds(0, NC)]
            pltpu.make_async_copy(blocks, blocks, relay_sem.at[slot]).wait()
            for c in range(NC):
                pltpu.make_async_remote_copy(
                    relay.at[slot * NC + c], recv.at[at(-dy, -dx) * NC + c], fsend_sem, recv_sem.at[single(DETOUR)],
                    device_id={"aa": to_plane}, device_id_type=MESH).start()

    own = CHIPS - 1
    one = recv.at[0]
    pltpu.make_async_copy(one, one, recv_sem.at[own_sem]).wait()
    block(own, chip)

    @pl.when(adds_up)
    def _():
        rows[pl.ds(plane * PEERS + me, 1), :] = part[pl.ds(own, 1), :]

    for p, c in ((0, ADDER), (1, ADDER), (0, 1 - ADDER)):
        there = jnp.logical_not((plane == p) & (core == c))
        if (p, c) != (0, ADDER):
            there = there & first_chips

        @pl.when(there)
        def _():
            give(own, {"aa": p, "ba": chip * NC + c})

    first = 0
    for g, end in enumerate(GROUPS):
        await_blocks(end - first, g)
        lax.fori_loop(first, end, use, 0)
        first = end
        for slot in range(slots):
            if end == PASS_AFTER[slot]:
                pass_on(slot)

    lax.fori_loop(first, DETOUR, arrive, 0)

    @pl.when(jnp.logical_not(detours))
    def _():
        arrive(DETOUR, 0)

    first = DETOUR + 1
    for end in (DETOUR_USE, len(ORDER)):
        if first < end:
            lax.fori_loop(first, end, arrive, 0)
            first = end
        if end == DETOUR_USE:
            @pl.when(detours)
            def _():
                arrive(DETOUR, 0)

    centre = jnp.sum(acc[...], axis=1, keepdims=True) * (1.0 / (CHIPS * LANES))
    a = inverse * (1.0 / KEEP_RATE)
    b = a * centre

    def finish(k, _):
        gin_ref[:, pl.ds(pl.multiple_of(k * LANES, LANES), LANES)] = (a * gs_ref[k] - b * n_ref[k]).astype(jnp.bfloat16)
        return 0

    lax.fori_loop(0, CHIPS, finish, 0)
    sent = recv.at[pl.ds(0, PEERS - 1)]
    pltpu.make_async_copy(sent, sent, send_sem).wait()

    for via in sorted({v for _, v, _ in DETOURS}):
        @pl.when(plane == via)
        def _():
            passed = relay.at[pl.ds(0, NC * sum(v == via for _, v, _ in DETOURS))]
            pltpu.make_async_copy(passed, passed, fsend_sem).wait()


    def tell(device):
        pltpu.make_async_remote_copy(
            share, share, tsend_sem, trecv_sem, device_id=device, device_id_type=MESH).start()

    def tell_plane(p, _):
        for c in (ADDER, 1 - ADDER):
            tell({"aa": p, "ba": chip * NC + c})
        return 0

    count = CHIPS + 2 * FIRST

    @pl.when(adds_up)
    def _():
        others = rows.at[pl.ds(0, planes * PEERS - 1)]
        pltpu.make_async_copy(others, others, rrecv_sem).wait()
        share[...] = jnp.sum(rows[...], axis=0, keepdims=True) * scale

        @pl.when(tells)
        def _():
            tell({"ba": me ^ 1})

        @pl.when(tells & first_plane)
        def _():
            lax.fori_loop(1, planes, tell_plane, 0)
            told = rows.at[pl.ds(0, planes * NC - 1)]
            pltpu.make_async_copy(told, told, tsend_sem).wait()

        @pl.when(tells & jnp.logical_not(first_plane))
        def _():
            lax.fori_loop(2, planes, tell_plane, 0)
            told = rows.at[pl.ds(0, (planes - 1) * NC - 1)]
            pltpu.make_async_copy(told, told, tsend_sem).wait()

        given = rows.at[pl.ds(0, count - 1)]
        pltpu.make_async_copy(given, given, rsend_sem).wait()

    @pl.when(jnp.logical_not(adds_up))
    def _():
        given = rows.at[pl.ds(0, count)]
        pltpu.make_async_copy(given, given, rsend_sem).wait()
        pltpu.make_async_copy(share, share, trecv_sem).wait()

    total_ref[...] = jnp.where(core == 0, share[:, :half], share[:, half:])


def write_kernel(gin_ref, total_ref, gin_hbm, gain_hbm, sems):
    copies = [pltpu.make_async_copy(gin_ref, gin_hbm, sems.at[0]), pltpu.make_async_copy(total_ref, gain_hbm, sems.at[1])]
    for copy in copies:
        copy.start()
    for copy in copies:
        copy.wait()


def per_device(planes, grad_out, saved_input, keep_bits, gain):
    rows, width = saved_input.shape
    tokens = grad_out.shape[0] * planes
    vmem = functools.partial(pl.BlockSpec, memory_space=pltpu.VMEM)
    hbm = functools.partial(pl.BlockSpec, memory_space=pltpu.HBM)
    f32 = jnp.float32
    grad_in = jax.ShapeDtypeStruct((rows, width), jnp.bfloat16)
    share = jax.ShapeDtypeStruct((1, LANES // NC), f32)
    blocks = pltpu.VMEM((CHIPS, LANES, LANES), f32)
    results = pl.pallas_call(
        functools.partial(exchange_kernel, planes, 1.0 / math.sqrt(tokens)),
        name="exchange",
        out_shape=(pltpu.VMEM(grad_in.shape, grad_in.dtype), pltpu.VMEM(share.shape, f32)),
        in_specs=[hbm(), hbm(), hbm(), hbm()],
        out_specs=(vmem(), vmem()),
        scratch_shapes=[
            pltpu.VMEM((LANES // NC, PEERS * LANES), jnp.bfloat16),
            pltpu.VMEM((rows, width), jnp.bfloat16),
            pltpu.VMEM(keep_bits.shape, jnp.int32),
            pltpu.VMEM((CHIPS, LANES), f32),
            pltpu.VMEM((PEERS, LANES // NC, LANES), jnp.bfloat16),
            blocks, blocks, blocks,
            pltpu.VMEM((CHIPS, LANES), f32),
            pltpu.VMEM((planes * PEERS, LANES), f32),
            pltpu.VMEM((1, LANES), f32),
            pltpu.VMEM((LANES, LANES), f32),
            pltpu.VMEM((NC * len(PASS_AFTER), LANES // NC, LANES), jnp.bfloat16),
            pltpu.SemaphoreType.DMA((4,)),
            pltpu.SemaphoreType.DMA,
            pltpu.SemaphoreType.DMA((SEMAPHORES,)),
            pltpu.SemaphoreType.DMA,
            pltpu.SemaphoreType.DMA,
            pltpu.SemaphoreType.DMA,
            pltpu.SemaphoreType.DMA,
            pltpu.SemaphoreType.REGULAR((NX - 1,)),
            pltpu.SemaphoreType.REGULAR,
            pltpu.SemaphoreType.REGULAR,
            pltpu.SemaphoreType.DMA((len(PASS_AFTER),)),
            pltpu.SemaphoreType.DMA,
        ],
        compiler_params=pltpu.CompilerParams(collective_id=0, has_side_effects=True, vmem_limit_bytes=24 << 20),
    )(*(pltpu.with_memory_space_constraint(a, pltpu.HBM) for a in (grad_out.T, saved_input, keep_bits, gain.reshape(CHIPS, LANES))))
    grad_in, share = pl.pallas_call(
        write_kernel,
        name="write",
        out_shape=(grad_in, share),
        in_specs=[vmem(), vmem()],
        out_specs=(hbm(), hbm()),
        scratch_shapes=[pltpu.SemaphoreType.DMA((2,))],
        compiler_params=pltpu.CompilerParams(vmem_limit_bytes=4 << 20),
    )(*results)
    return grad_in, share.reshape(LANES // NC)


def solution(mesh):
    placed = (P("aa", "ba"), P(("aa", "ba"), None), P(("aa", "ba"), None), P())
    return jax.shard_map(
        functools.partial(per_device, mesh.shape["aa"]),
        mesh=mesh,
        in_specs=placed,
        out_specs=(P(("aa", "ba"), None), P("ba")),
        check_vma=False,
    )
```

```python
import functools
import math

import jax
import jax.numpy as jnp
from jax import lax
from jax.experimental import pallas as pl
from jax.experimental.pallas import tpu as pltpu
from jax.sharding import PartitionSpec as P

KEEP_RATE = 0.9
EPSILON = 1e-06
MESH = pl.DeviceIdType.MESH
LANES = 128
NY, NX, NC = 8, 4, 2
CHIPS = NY * NX
PEERS = CHIPS * NC


FAR, NEAR = (4, 3, 5), (2, 6, 1, 7)
ORDER = (
    tuple((y, 0) for y in FAR)
    + ((0, 2), (0, 1), (0, 3))
    + tuple((y, 2) for y in FAR + NEAR)
    + tuple((y, 1) for y in FAR + NEAR)
    + tuple((y, 3) for y in FAR + NEAR)
    + tuple((y, 0) for y in NEAR)
)
HEAD = len(FAR)
ADDER = 1
FIRST = 2 * NX
GROUPS = (6, 13, 20)
SEMAPHORES = len(GROUPS) + len(ORDER) - GROUPS[-1] + 1
DETOUR = 20
DETOURS = ((7, 3, 0), (6, 2, 0), (8, 4, 0))
PASS_AFTER = (6, 13, 20)
DETOUR_USE = 21
PER_WORD = 6


def offset(r):
    codes = [dy * NX + dx for dy, dx in ORDER]
    words = [sum(c << (5 * i) for i, c in enumerate(codes[w:w + PER_WORD])) for w in range(0, len(codes), PER_WORD)]
    group = r // PER_WORD
    word = jnp.int32(words[0])
    for g, w in enumerate(words[1:], 1):
        word = jnp.where(group >= g, jnp.int32(w), word)
    code = (word >> (5 * (r - group * PER_WORD))) & (CHIPS - 1)
    return code >> 2, code & (NX - 1)


def exchange_kernel(
    planes, scale,
    gt_hbm, x_hbm, kb_hbm, gain_hbm, gin_ref, total_ref,
    gt_ref, x_ref, kb_ref, gain_ref, recv, keep_ref, n_ref, gs_ref, part, rows, share, acc, relay,
    in_sem, send_sem, recv_sem, rsend_sem, rrecv_sem, tsend_sem, trecv_sem, row_sem, up_sem, low_sem, relay_sem, fsend_sem,
):
    me = lax.axis_index("ba")
    plane = lax.axis_index("aa")
    core = me & 1
    chip = me >> 1
    my_y, my_x = chip >> 2, chip & (NX - 1)
    half = LANES // NC
    first_plane, last_plane = plane == 0, plane == planes - 1
    adder, first_chips = core == ADDER, chip < FIRST
    alone = first_plane & first_chips
    tells = adder & (first_plane & jnp.logical_not(first_chips) | (plane == 1) & first_chips)
    adds_up = alone | tells

    def at(dy, dx=0):
        return ((my_y + dy) & (NY - 1)) * NX + ((my_x + dx) & (NX - 1))

    def above(dz):
        return {"aa": lax.rem(plane + dz + planes, planes)}

    def signal(sem, device, inc=1):
        pl.semaphore_signal(sem, inc=inc, device_id=device, device_id_type=MESH)

    barrier = pltpu.get_barrier_semaphore()
    for dy in (4, 3, 5, 2, 6, 1, 7):
        for c in range(NC):
            signal(barrier, {"ba": at(dy) * NC + c})
    for dx in (2, 1, 3):
        signal(barrier, {"ba": at(0, dx) * NC + core})
    signal(barrier, {"ba": me ^ 1})

    @pl.when(jnp.logical_not(last_plane))
    def _():
        signal(barrier, above(1))

    loads = [
        pltpu.make_async_copy(source, target, in_sem.at[i])
        for i, (source, target) in enumerate(((gt_hbm, gt_ref), (x_hbm, x_ref), (kb_hbm, kb_ref), (gain_hbm, gain_ref)))
    ]
    for load in loads:
        load.start()
    near = (NY - 1) * NC + (NX - 1) + 1
    loads[0].wait()
    pl.semaphore_wait(barrier, jnp.where(first_plane, near, jnp.where(last_plane, near + 2, near + 1)))

    def bulk(dst, sem):
        pltpu.make_async_remote_copy(
            gt_ref.at[:, pl.ds(pl.multiple_of(dst * LANES, LANES), LANES)],
            recv.at[me], send_sem, recv_sem.at[sem],
            device_id={"ba": dst}, device_id_type=MESH).start()

    def serve(first, end, sem):
        def send(r, _):
            to = at(*offset(r)) * NC
            for c in range(NC):
                bulk(to + c, sem(r))
            return 0

        lax.fori_loop(first, end, send, 0)

    def single(r):
        return r - GROUPS[-1] + len(GROUPS)

    own_sem = SEMAPHORES - 1

    for dx in (2, 1, 3):
        signal(row_sem.at[dx - 1], {"ba": at(0, -dx) * NC + core})
    serve(0, HEAD, lambda r: 0)
    bulk(me ^ 1, own_sem)
    for dx in (1, 3, 2):
        pl.semaphore_wait(row_sem.at[dx - 1], 1)
    first = HEAD
    for g, end in enumerate(GROUPS):
        serve(first, end, lambda r: g)
        first = end
    slots = max(s for _, _, s in DETOURS) + 1
    detours, via_plane, my_slot = False, plane, 0
    for late, via, slot in DETOURS:
        detours = detours | (plane == late)
        via_plane = jnp.where(plane == late, via, via_plane)
        my_slot = jnp.where(plane == late, slot, my_slot)
    serve(first, DETOUR, single)

    @pl.when(jnp.logical_not(detours))
    def _():
        serve(DETOUR, DETOUR + 1, single)

    serve(DETOUR + 1, len(ORDER), single)

    homes = 2
    inner = jnp.logical_not(first_plane | last_plane)

    @pl.when(plane < homes - 1)
    def _():
        pl.semaphore_wait(up_sem, 1)

    @pl.when(inner)
    def _():
        signal(up_sem, above(-1))

    @pl.when(first_plane)
    def _():
        signal(low_sem, above(1))
        signal(barrier, above(-1))

    lane = lax.broadcasted_iota(jnp.int32, (LANES, LANES), 1)
    word = lane >> 5
    shift = 31 - (lane & 31)
    for load in loads[1:]:
        load.wait()
    recv[me] = gt_ref[:, pl.ds(pl.multiple_of(me * LANES, LANES), LANES)]
    acc[...] = jnp.zeros_like(acc)

    def forward(k, _):
        x = x_ref[:, pl.ds(pl.multiple_of(k * LANES, LANES), LANES)].astype(jnp.float32)
        words = jnp.take_along_axis(kb_ref[...], word + 4 * k, axis=1)
        keep = jnp.where(jnp.left_shift(words, shift) < 0, 1.0, 0.0)
        dropped = x * keep * (1.0 / KEEP_RATE)
        keep_ref[k] = keep
        n_ref[k] = dropped
        acc[...] += dropped * dropped
        return 0

    lax.fori_loop(0, CHIPS, forward, 0)
    mean = jnp.sum(acc[...], axis=1, keepdims=True) * (1.0 / (CHIPS * LANES))
    inverse = lax.rsqrt(mean + EPSILON)

    def normalise(k, _):
        n_ref[k] = n_ref[k] * inverse
        return 0

    lax.fori_loop(0, CHIPS, normalise, 0)
    acc[...] = jnp.zeros_like(acc)

    def block(r, k):
        grads = recv[pl.ds(k * NC, NC)].reshape(LANES, LANES).astype(jnp.float32).T
        grads = grads * keep_ref[k]
        normed = n_ref[k]
        part[pl.ds(r, 1), :] = jnp.sum(grads * normed, axis=0, keepdims=True)
        scaled = grads * gain_ref[pl.ds(k, 1), :]
        gs_ref[k] = scaled
        acc[...] += scaled * normed

    def give(r, device):
        pltpu.make_async_remote_copy(
            part.at[pl.ds(r, 1)], rows.at[pl.ds(plane * PEERS + me, 1)], rsend_sem, rrecv_sem,
            device_id=device, device_id_type=MESH).start()

    def give_back(r, k):
        give(r, {"aa": 0, "ba": k * NC + ADDER})

        @pl.when(k < FIRST)
        def _():
            give(r, {"aa": 1, "ba": k * NC + ADDER})
            give(r, {"aa": 0, "ba": k * NC + 1 - ADDER})

    def await_blocks(chips, sem):
        blocks = recv.at[pl.ds(0, chips * NC)]
        pltpu.make_async_copy(blocks, blocks, recv_sem.at[sem]).wait()

    def use(r, _):
        dy, dx = offset(r)
        k = at(-dy, -dx)
        block(r, k)
        give_back(r, k)
        return 0

    def arrive(r, _):
        await_blocks(1, single(r))
        return use(r, 0)

    @pl.when((plane >= homes - 1) & (plane < planes - 2))
    def _():
        pl.semaphore_wait(up_sem, 1)

    @pl.when(inner)
    def _():
        pl.semaphore_wait(low_sem, 1)

    @pl.when(inner & (plane < planes - 2))
    def _():
        signal(low_sem, above(1))

    dy, dx = ORDER[DETOUR]

    @pl.when(detours)
    def _():
        to = at(dy, dx) * NC
        for c in range(NC):
            pltpu.make_async_remote_copy(
                gt_ref.at[:, pl.ds(pl.multiple_of((to + c) * LANES, LANES), LANES)],
                relay.at[my_slot * NC + core], send_sem, relay_sem.at[my_slot],
                device_id={"aa": via_plane, "ba": to + c}, device_id_type=MESH).start()

    def pass_on(slot):
        passes, to_plane = False, plane
        for late, via, there in DETOURS:
            if there == slot:
                passes = passes | (plane == via)
                to_plane = jnp.where(plane == via, late, to_plane)

        @pl.when(passes)
        def _():
            blocks = relay.at[pl.ds(0, NC)]
            pltpu.make_async_copy(blocks, blocks, relay_sem.at[slot]).wait()
            for c in range(NC):
                pltpu.make_async_remote_copy(
                    relay.at[slot * NC + c], recv.at[at(-dy, -dx) * NC + c], fsend_sem, recv_sem.at[single(DETOUR)],
                    device_id={"aa": to_plane}, device_id_type=MESH).start()

    own = CHIPS - 1
    one = recv.at[0]
    pltpu.make_async_copy(one, one, recv_sem.at[own_sem]).wait()
    block(own, chip)

    @pl.when(adds_up)
    def _():
        rows[pl.ds(plane * PEERS + me, 1), :] = part[pl.ds(own, 1), :]

    for p, c in ((0, ADDER), (1, ADDER), (0, 1 - ADDER)):
        there = jnp.logical_not((plane == p) & (core == c))
        if (p, c) != (0, ADDER):
            there = there & first_chips

        @pl.when(there)
        def _():
            give(own, {"aa": p, "ba": chip * NC + c})

    first = 0
    for g, end in enumerate(GROUPS):
        await_blocks(end - first, g)
        lax.fori_loop(first, end, use, 0)
        first = end
        for slot in range(slots):
            if end == PASS_AFTER[slot]:
                pass_on(slot)

    lax.fori_loop(first, DETOUR, arrive, 0)

    @pl.when(jnp.logical_not(detours))
    def _():
        arrive(DETOUR, 0)

    first = DETOUR + 1
    for end in (DETOUR_USE, len(ORDER)):
        if first < end:
            lax.fori_loop(first, end, arrive, 0)
            first = end
        if end == DETOUR_USE:
            @pl.when(detours)
            def _():
                arrive(DETOUR, 0)

    centre = jnp.sum(acc[...], axis=1, keepdims=True) * (1.0 / (CHIPS * LANES))
    a = inverse * (1.0 / KEEP_RATE)
    b = a * centre

    def finish(k, _):
        gin_ref[:, pl.ds(pl.multiple_of(k * LANES, LANES), LANES)] = (a * gs_ref[k] - b * n_ref[k]).astype(jnp.bfloat16)
        return 0

    lax.fori_loop(0, CHIPS, finish, 0)
    sent = recv.at[pl.ds(0, PEERS - 1)]
    pltpu.make_async_copy(sent, sent, send_sem).wait()

    for via in sorted({v for _, v, _ in DETOURS}):
        @pl.when(plane == via)
        def _():
            passed = relay.at[pl.ds(0, NC * sum(v == via for _, v, _ in DETOURS))]
            pltpu.make_async_copy(passed, passed, fsend_sem).wait()


    def tell(device):
        pltpu.make_async_remote_copy(
            share, share, tsend_sem, trecv_sem, device_id=device, device_id_type=MESH).start()

    def tell_plane(p, _):
        for c in (ADDER, 1 - ADDER):
            tell({"aa": p, "ba": chip * NC + c})
        return 0

    count = CHIPS + 2 * FIRST

    @pl.when(adds_up)
    def _():
        others = rows.at[pl.ds(0, planes * PEERS - 1)]
        pltpu.make_async_copy(others, others, rrecv_sem).wait()
        share[...] = jnp.sum(rows[...], axis=0, keepdims=True) * scale

        @pl.when(tells)
        def _():
            tell({"ba": me ^ 1})

        @pl.when(tells & first_plane)
        def _():
            lax.fori_loop(1, planes, tell_plane, 0)
            told = rows.at[pl.ds(0, planes * NC - 1)]
            pltpu.make_async_copy(told, told, tsend_sem).wait()

        @pl.when(tells & jnp.logical_not(first_plane))
        def _():
            lax.fori_loop(2, planes, tell_plane, 0)
            told = rows.at[pl.ds(0, (planes - 1) * NC - 1)]
            pltpu.make_async_copy(told, told, tsend_sem).wait()

        given = rows.at[pl.ds(0, count - 1)]
        pltpu.make_async_copy(given, given, rsend_sem).wait()

    @pl.when(jnp.logical_not(adds_up))
    def _():
        given = rows.at[pl.ds(0, count)]
        pltpu.make_async_copy(given, given, rsend_sem).wait()
        pltpu.make_async_copy(share, share, trecv_sem).wait()

    total_ref[...] = jnp.where(core == 0, share[:, :half], share[:, half:])


def write_kernel(gin_ref, total_ref, gin_hbm, gain_hbm, sems):
    copies = [pltpu.make_async_copy(gin_ref, gin_hbm, sems.at[0]), pltpu.make_async_copy(total_ref, gain_hbm, sems.at[1])]
    for copy in copies:
        copy.start()
    for copy in copies:
        copy.wait()


def per_device(planes, grad_out, saved_input, keep_bits, gain):
    rows, width = saved_input.shape
    tokens = grad_out.shape[0] * planes
    vmem = functools.partial(pl.BlockSpec, memory_space=pltpu.VMEM)
    hbm = functools.partial(pl.BlockSpec, memory_space=pltpu.HBM)
    f32 = jnp.float32
    grad_in = jax.ShapeDtypeStruct((rows, width), jnp.bfloat16)
    share = jax.ShapeDtypeStruct((1, LANES // NC), f32)
    blocks = pltpu.VMEM((CHIPS, LANES, LANES), f32)
    results = pl.pallas_call(
        functools.partial(exchange_kernel, planes, 1.0 / math.sqrt(tokens)),
        name="exchange",
        out_shape=(pltpu.VMEM(grad_in.shape, grad_in.dtype), pltpu.VMEM(share.shape, f32)),
        in_specs=[hbm(), hbm(), hbm(), hbm()],
        out_specs=(vmem(), vmem()),
        scratch_shapes=[
            pltpu.VMEM((LANES // NC, PEERS * LANES), jnp.bfloat16),
            pltpu.VMEM((rows, width), jnp.bfloat16),
            pltpu.VMEM(keep_bits.shape, jnp.int32),
            pltpu.VMEM((CHIPS, LANES), f32),
            pltpu.VMEM((PEERS, LANES // NC, LANES), jnp.bfloat16),
            blocks, blocks, blocks,
            pltpu.VMEM((CHIPS, LANES), f32),
            pltpu.VMEM((planes * PEERS, LANES), f32),
            pltpu.VMEM((1, LANES), f32),
            pltpu.VMEM((LANES, LANES), f32),
            pltpu.VMEM((NC * len(PASS_AFTER), LANES // NC, LANES), jnp.bfloat16),
            pltpu.SemaphoreType.DMA((4,)),
            pltpu.SemaphoreType.DMA,
            pltpu.SemaphoreType.DMA((SEMAPHORES,)),
            pltpu.SemaphoreType.DMA,
            pltpu.SemaphoreType.DMA,
            pltpu.SemaphoreType.DMA,
            pltpu.SemaphoreType.DMA,
            pltpu.SemaphoreType.REGULAR((NX - 1,)),
            pltpu.SemaphoreType.REGULAR,
            pltpu.SemaphoreType.REGULAR,
            pltpu.SemaphoreType.DMA((len(PASS_AFTER),)),
            pltpu.SemaphoreType.DMA,
        ],
        compiler_params=pltpu.CompilerParams(collective_id=0, has_side_effects=True, vmem_limit_bytes=24 << 20),
    )(*(pltpu.with_memory_space_constraint(a, pltpu.HBM) for a in (grad_out.T, saved_input, keep_bits, gain.reshape(CHIPS, LANES))))
    grad_in, share = pl.pallas_call(
        write_kernel,
        name="write",
        out_shape=(grad_in, share),
        in_specs=[vmem(), vmem()],
        out_specs=(hbm(), hbm()),
        scratch_shapes=[pltpu.SemaphoreType.DMA((2,))],
        compiler_params=pltpu.CompilerParams(vmem_limit_bytes=4 << 20),
    )(*results)
    return grad_in, share.reshape(LANES // NC)


def solution(mesh):
    placed = (P("aa", "ba"), P(("aa", "ba"), None), P(("aa", "ba"), None), P())
    return jax.shard_map(
        functools.partial(per_device, mesh.shape["aa"]),
        mesh=mesh,
        in_specs=placed,
        out_specs=(P(("aa", "ba"), None), P("ba")),
        check_vma=False,
    )
```

```python
import functools
import math

import jax
import jax.numpy as jnp
from jax import lax
from jax.experimental import pallas as pl
from jax.experimental.pallas import tpu as pltpu
from jax.sharding import PartitionSpec as P

KEEP_RATE = 0.9
EPSILON = 1e-06
MESH = pl.DeviceIdType.MESH
LANES = 128
NY, NX, NC = 8, 4, 2
CHIPS = NY * NX
PEERS = CHIPS * NC


FAR, NEAR = (4, 3, 5), (2, 6, 1, 7)
ORDER = (
    tuple((y, 0) for y in FAR)
    + ((0, 2), (0, 1), (0, 3))
    + tuple((y, 2) for y in FAR + NEAR)
    + tuple((y, 1) for y in FAR + NEAR)
    + tuple((y, 3) for y in FAR + NEAR)
    + tuple((y, 0) for y in NEAR)
)
HEAD = len(FAR)
ADDER = 1
FIRST = 2 * NX
GROUPS = (6, 13, 20)
SEMAPHORES = len(GROUPS) + len(ORDER) - GROUPS[-1] + 1
DETOUR = 20
DETOURS = ((7, 4, 0), (6, 3, 0))
PASS_AFTER = (6, 13, 20)
DETOUR_USE = 21
PER_WORD = 6


def offset(r):
    codes = [dy * NX + dx for dy, dx in ORDER]
    words = [sum(c << (5 * i) for i, c in enumerate(codes[w:w + PER_WORD])) for w in range(0, len(codes), PER_WORD)]
    group = r // PER_WORD
    word = jnp.int32(words[0])
    for g, w in enumerate(words[1:], 1):
        word = jnp.where(group >= g, jnp.int32(w), word)
    code = (word >> (5 * (r - group * PER_WORD))) & (CHIPS - 1)
    return code >> 2, code & (NX - 1)


def exchange_kernel(
    planes, scale,
    gt_hbm, x_hbm, kb_hbm, gain_hbm, gin_ref, total_ref,
    gt_ref, x_ref, kb_ref, gain_ref, recv, keep_ref, n_ref, gs_ref, part, rows, share, acc, relay,
    in_sem, send_sem, recv_sem, rsend_sem, rrecv_sem, tsend_sem, trecv_sem, row_sem, up_sem, low_sem, relay_sem, fsend_sem,
):
    me = lax.axis_index("ba")
    plane = lax.axis_index("aa")
    core = me & 1
    chip = me >> 1
    my_y, my_x = chip >> 2, chip & (NX - 1)
    half = LANES // NC
    first_plane, last_plane = plane == 0, plane == planes - 1
    adder, first_chips = core == ADDER, chip < FIRST
    alone = first_plane & first_chips
    tells = adder & (first_plane & jnp.logical_not(first_chips) | (plane == 1) & first_chips)
    adds_up = alone | tells

    def at(dy, dx=0):
        return ((my_y + dy) & (NY - 1)) * NX + ((my_x + dx) & (NX - 1))

    def above(dz):
        return {"aa": lax.rem(plane + dz + planes, planes)}

    def signal(sem, device, inc=1):
        pl.semaphore_signal(sem, inc=inc, device_id=device, device_id_type=MESH)

    barrier = pltpu.get_barrier_semaphore()
    for dy in (4, 3, 5, 2, 6, 1, 7):
        for c in range(NC):
            signal(barrier, {"ba": at(dy) * NC + c})
    for dx in (2, 1, 3):
        signal(barrier, {"ba": at(0, dx) * NC + core})
    signal(barrier, {"ba": me ^ 1})

    @pl.when(jnp.logical_not(last_plane))
    def _():
        signal(barrier, above(1))

    loads = [
        pltpu.make_async_copy(source, target, in_sem.at[i])
        for i, (source, target) in enumerate(((gt_hbm, gt_ref), (x_hbm, x_ref), (kb_hbm, kb_ref), (gain_hbm, gain_ref)))
    ]
    for load in loads:
        load.start()
    near = (NY - 1) * NC + (NX - 1) + 1
    loads[0].wait()
    pl.semaphore_wait(barrier, jnp.where(first_plane, near, jnp.where(last_plane, near + 2, near + 1)))

    def bulk(dst, sem):
        pltpu.make_async_remote_copy(
            gt_ref.at[:, pl.ds(pl.multiple_of(dst * LANES, LANES), LANES)],
            recv.at[me], send_sem, recv_sem.at[sem],
            device_id={"ba": dst}, device_id_type=MESH).start()

    def serve(first, end, sem):
        def send(r, _):
            to = at(*offset(r)) * NC
            for c in range(NC):
                bulk(to + c, sem(r))
            return 0

        lax.fori_loop(first, end, send, 0)

    def single(r):
        return r - GROUPS[-1] + len(GROUPS)

    own_sem = SEMAPHORES - 1

    for dx in (2, 1, 3):
        signal(row_sem.at[dx - 1], {"ba": at(0, -dx) * NC + core})
    serve(0, HEAD, lambda r: 0)
    bulk(me ^ 1, own_sem)
    for dx in (1, 3, 2):
        pl.semaphore_wait(row_sem.at[dx - 1], 1)
    first = HEAD
    for g, end in enumerate(GROUPS):
        serve(first, end, lambda r: g)
        first = end
    slots = max(s for _, _, s in DETOURS) + 1
    detours, via_plane, my_slot = False, plane, 0
    for late, via, slot in DETOURS:
        detours = detours | (plane == late)
        via_plane = jnp.where(plane == late, via, via_plane)
        my_slot = jnp.where(plane == late, slot, my_slot)
    serve(first, DETOUR, single)

    @pl.when(jnp.logical_not(detours))
    def _():
        serve(DETOUR, DETOUR + 1, single)

    serve(DETOUR + 1, len(ORDER), single)

    homes = 2
    inner = jnp.logical_not(first_plane | last_plane)

    @pl.when(plane < homes - 1)
    def _():
        pl.semaphore_wait(up_sem, 1)

    @pl.when(inner)
    def _():
        signal(up_sem, above(-1))

    @pl.when(first_plane)
    def _():
        signal(low_sem, above(1))
        signal(barrier, above(-1))

    lane = lax.broadcasted_iota(jnp.int32, (LANES, LANES), 1)
    word = lane >> 5
    shift = 31 - (lane & 31)
    for load in loads[1:]:
        load.wait()
    recv[me] = gt_ref[:, pl.ds(pl.multiple_of(me * LANES, LANES), LANES)]
    acc[...] = jnp.zeros_like(acc)

    def forward(k, _):
        x = x_ref[:, pl.ds(pl.multiple_of(k * LANES, LANES), LANES)].astype(jnp.float32)
        words = jnp.take_along_axis(kb_ref[...], word + 4 * k, axis=1)
        keep = jnp.where(jnp.left_shift(words, shift) < 0, 1.0, 0.0)
        dropped = x * keep * (1.0 / KEEP_RATE)
        keep_ref[k] = keep
        n_ref[k] = dropped
        acc[...] += dropped * dropped
        return 0

    lax.fori_loop(0, CHIPS, forward, 0)
    mean = jnp.sum(acc[...], axis=1, keepdims=True) * (1.0 / (CHIPS * LANES))
    inverse = lax.rsqrt(mean + EPSILON)

    def normalise(k, _):
        n_ref[k] = n_ref[k] * inverse
        return 0

    lax.fori_loop(0, CHIPS, normalise, 0)
    acc[...] = jnp.zeros_like(acc)

    def block(r, k):
        grads = recv[pl.ds(k * NC, NC)].reshape(LANES, LANES).astype(jnp.float32).T
        grads = grads * keep_ref[k]
        normed = n_ref[k]
        part[pl.ds(r, 1), :] = jnp.sum(grads * normed, axis=0, keepdims=True)
        scaled = grads * gain_ref[pl.ds(k, 1), :]
        gs_ref[k] = scaled
        acc[...] += scaled * normed

    def give(r, device):
        pltpu.make_async_remote_copy(
            part.at[pl.ds(r, 1)], rows.at[pl.ds(plane * PEERS + me, 1)], rsend_sem, rrecv_sem,
            device_id=device, device_id_type=MESH).start()

    def give_back(r, k):
        give(r, {"aa": 0, "ba": k * NC + ADDER})

        @pl.when(k < FIRST)
        def _():
            give(r, {"aa": 1, "ba": k * NC + ADDER})
            give(r, {"aa": 0, "ba": k * NC + 1 - ADDER})

    def await_blocks(chips, sem):
        blocks = recv.at[pl.ds(0, chips * NC)]
        pltpu.make_async_copy(blocks, blocks, recv_sem.at[sem]).wait()

    def use(r, _):
        dy, dx = offset(r)
        k = at(-dy, -dx)
        block(r, k)
        give_back(r, k)
        return 0

    def arrive(r, _):
        await_blocks(1, single(r))
        return use(r, 0)

    @pl.when((plane >= homes - 1) & (plane < planes - 2))
    def _():
        pl.semaphore_wait(up_sem, 1)

    @pl.when(inner)
    def _():
        pl.semaphore_wait(low_sem, 1)

    @pl.when(inner & (plane < planes - 2))
    def _():
        signal(low_sem, above(1))

    dy, dx = ORDER[DETOUR]

    @pl.when(detours)
    def _():
        to = at(dy, dx) * NC
        for c in range(NC):
            pltpu.make_async_remote_copy(
                gt_ref.at[:, pl.ds(pl.multiple_of((to + c) * LANES, LANES), LANES)],
                relay.at[my_slot * NC + core], send_sem, relay_sem.at[my_slot],
                device_id={"aa": via_plane, "ba": to + c}, device_id_type=MESH).start()

    def pass_on(slot):
        passes, to_plane = False, plane
        for late, via, there in DETOURS:
            if there == slot:
                passes = passes | (plane == via)
                to_plane = jnp.where(plane == via, late, to_plane)

        @pl.when(passes)
        def _():
            blocks = relay.at[pl.ds(0, NC)]
            pltpu.make_async_copy(blocks, blocks, relay_sem.at[slot]).wait()
            for c in range(NC):
                pltpu.make_async_remote_copy(
                    relay.at[slot * NC + c], recv.at[at(-dy, -dx) * NC + c], fsend_sem, recv_sem.at[single(DETOUR)],
                    device_id={"aa": to_plane}, device_id_type=MESH).start()

    own = CHIPS - 1
    one = recv.at[0]
    pltpu.make_async_copy(one, one, recv_sem.at[own_sem]).wait()
    block(own, chip)

    @pl.when(adds_up)
    def _():
        rows[pl.ds(plane * PEERS + me, 1), :] = part[pl.ds(own, 1), :]

    for p, c in ((0, ADDER), (1, ADDER), (0, 1 - ADDER)):
        there = jnp.logical_not((plane == p) & (core == c))
        if (p, c) != (0, ADDER):
            there = there & first_chips

        @pl.when(there)
        def _():
            give(own, {"aa": p, "ba": chip * NC + c})

    first = 0
    for g, end in enumerate(GROUPS):
        await_blocks(end - first, g)
        lax.fori_loop(first, end, use, 0)
        first = end
        for slot in range(slots):
            if end == PASS_AFTER[slot]:
                pass_on(slot)

    lax.fori_loop(first, DETOUR, arrive, 0)

    @pl.when(jnp.logical_not(detours))
    def _():
        arrive(DETOUR, 0)

    first = DETOUR + 1
    for end in (DETOUR_USE, len(ORDER)):
        if first < end:
            lax.fori_loop(first, end, arrive, 0)
            first = end
        if end == DETOUR_USE:
            @pl.when(detours)
            def _():
                arrive(DETOUR, 0)

    centre = jnp.sum(acc[...], axis=1, keepdims=True) * (1.0 / (CHIPS * LANES))
    a = inverse * (1.0 / KEEP_RATE)
    b = a * centre

    def finish(k, _):
        gin_ref[:, pl.ds(pl.multiple_of(k * LANES, LANES), LANES)] = (a * gs_ref[k] - b * n_ref[k]).astype(jnp.bfloat16)
        return 0

    lax.fori_loop(0, CHIPS, finish, 0)
    sent = recv.at[pl.ds(0, PEERS - 1)]
    pltpu.make_async_copy(sent, sent, send_sem).wait()

    for via in sorted({v for _, v, _ in DETOURS}):
        @pl.when(plane == via)
        def _():
            passed = relay.at[pl.ds(0, NC * sum(v == via for _, v, _ in DETOURS))]
            pltpu.make_async_copy(passed, passed, fsend_sem).wait()


    def tell(device):
        pltpu.make_async_remote_copy(
            share, share, tsend_sem, trecv_sem, device_id=device, device_id_type=MESH).start()

    def tell_plane(p, _):
        for c in (ADDER, 1 - ADDER):
            tell({"aa": p, "ba": chip * NC + c})
        return 0

    count = CHIPS + 2 * FIRST

    @pl.when(adds_up)
    def _():
        others = rows.at[pl.ds(0, planes * PEERS - 1)]
        pltpu.make_async_copy(others, others, rrecv_sem).wait()
        share[...] = jnp.sum(rows[...], axis=0, keepdims=True) * scale

        @pl.when(tells)
        def _():
            tell({"ba": me ^ 1})

        @pl.when(tells & first_plane)
        def _():
            lax.fori_loop(1, planes, tell_plane, 0)
            told = rows.at[pl.ds(0, planes * NC - 1)]
            pltpu.make_async_copy(told, told, tsend_sem).wait()

        @pl.when(tells & jnp.logical_not(first_plane))
        def _():
            lax.fori_loop(2, planes, tell_plane, 0)
            told = rows.at[pl.ds(0, (planes - 1) * NC - 1)]
            pltpu.make_async_copy(told, told, tsend_sem).wait()

        given = rows.at[pl.ds(0, count - 1)]
        pltpu.make_async_copy(given, given, rsend_sem).wait()

    @pl.when(jnp.logical_not(adds_up))
    def _():
        given = rows.at[pl.ds(0, count)]
        pltpu.make_async_copy(given, given, rsend_sem).wait()
        pltpu.make_async_copy(share, share, trecv_sem).wait()

    total_ref[...] = jnp.where(core == 0, share[:, :half], share[:, half:])


def write_kernel(gin_ref, total_ref, gin_hbm, gain_hbm, sems):
    copies = [pltpu.make_async_copy(gin_ref, gin_hbm, sems.at[0]), pltpu.make_async_copy(total_ref, gain_hbm, sems.at[1])]
    for copy in copies:
        copy.start()
    for copy in copies:
        copy.wait()


def per_device(planes, grad_out, saved_input, keep_bits, gain):
    rows, width = saved_input.shape
    tokens = grad_out.shape[0] * planes
    vmem = functools.partial(pl.BlockSpec, memory_space=pltpu.VMEM)
    hbm = functools.partial(pl.BlockSpec, memory_space=pltpu.HBM)
    f32 = jnp.float32
    grad_in = jax.ShapeDtypeStruct((rows, width), jnp.bfloat16)
    share = jax.ShapeDtypeStruct((1, LANES // NC), f32)
    blocks = pltpu.VMEM((CHIPS, LANES, LANES), f32)
    results = pl.pallas_call(
        functools.partial(exchange_kernel, planes, 1.0 / math.sqrt(tokens)),
        name="exchange",
        out_shape=(pltpu.VMEM(grad_in.shape, grad_in.dtype), pltpu.VMEM(share.shape, f32)),
        in_specs=[hbm(), hbm(), hbm(), hbm()],
        out_specs=(vmem(), vmem()),
        scratch_shapes=[
            pltpu.VMEM((LANES // NC, PEERS * LANES), jnp.bfloat16),
            pltpu.VMEM((rows, width), jnp.bfloat16),
            pltpu.VMEM(keep_bits.shape, jnp.int32),
            pltpu.VMEM((CHIPS, LANES), f32),
            pltpu.VMEM((PEERS, LANES // NC, LANES), jnp.bfloat16),
            blocks, blocks, blocks,
            pltpu.VMEM((CHIPS, LANES), f32),
            pltpu.VMEM((planes * PEERS, LANES), f32),
            pltpu.VMEM((1, LANES), f32),
            pltpu.VMEM((LANES, LANES), f32),
            pltpu.VMEM((NC * len(PASS_AFTER), LANES // NC, LANES), jnp.bfloat16),
            pltpu.SemaphoreType.DMA((4,)),
            pltpu.SemaphoreType.DMA,
            pltpu.SemaphoreType.DMA((SEMAPHORES,)),
            pltpu.SemaphoreType.DMA,
            pltpu.SemaphoreType.DMA,
            pltpu.SemaphoreType.DMA,
            pltpu.SemaphoreType.DMA,
            pltpu.SemaphoreType.REGULAR((NX - 1,)),
            pltpu.SemaphoreType.REGULAR,
            pltpu.SemaphoreType.REGULAR,
            pltpu.SemaphoreType.DMA((len(PASS_AFTER),)),
            pltpu.SemaphoreType.DMA,
        ],
        compiler_params=pltpu.CompilerParams(collective_id=0, has_side_effects=True, vmem_limit_bytes=24 << 20),
    )(*(pltpu.with_memory_space_constraint(a, pltpu.HBM) for a in (grad_out.T, saved_input, keep_bits, gain.reshape(CHIPS, LANES))))
    grad_in, share = pl.pallas_call(
        write_kernel,
        name="write",
        out_shape=(grad_in, share),
        in_specs=[vmem(), vmem()],
        out_specs=(hbm(), hbm()),
        scratch_shapes=[pltpu.SemaphoreType.DMA((2,))],
        compiler_params=pltpu.CompilerParams(vmem_limit_bytes=4 << 20),
    )(*results)
    return grad_in, share.reshape(LANES // NC)


def solution(mesh):
    placed = (P("aa", "ba"), P(("aa", "ba"), None), P(("aa", "ba"), None), P())
    return jax.shard_map(
        functools.partial(per_device, mesh.shape["aa"]),
        mesh=mesh,
        in_specs=placed,
        out_specs=(P(("aa", "ba"), None), P("ba")),
        check_vma=False,
    )
```
